128 devices in a mesh: rows: 4 (over y_lo, core), cols: 32 (over z, x, y_hi).
Axes of the slice: x: 4, y: 4 (y_hi: 2, y_lo: 2; y = y_hi * 2 + y_lo), z: 4, core: 2. Of those that a mesh axis runs over, the one named last changes fastest.
Arguments:
- object_field: float32 [2, 512, 4096], P(None, 'rows', 'cols'), may hold values from -6 to 6
- probe: float32 [2, 256, 256], replicated, may hold values from -6 to 6
- amplitudes: float32 [4, 32, 4, 256, 256], P('rows', 'cols'), may hold values from 0.5 to 4
- offsets: int32 [4, 32, 4, 2], P('rows', 'cols'), may hold values from 0 to 128
Outputs:
- updated: float32 [2, 512, 4096], P(None, 'rows', 'cols')
The draws below stay inside these ranges and needn't reach their ends.
Inputs may be any that keep to these rules, and one draw needn't show every extreme that they name: `offsets`: every window lies inside its tile's extended region of 384 cells a side.
All inputs are finite; a program needn't handle non-finite values.
Results may differ from the reference program's by a relative error of at most 0.0001.
Values sent between devices are 32-bit elements; how exact they have to be, the bound alone decides.
A program may use at most 64 MiB of HBM per device.

```python
import math
import jax
import jax.numpy as jnp
from jax import lax

OWN = 128
WIN = 256
POS = 4
ITERS = 2
TR = 4
TC = 32
NR = 512
NC = 4096


def set_ends(values, stream_key, low, high):
    spot = [jax.random.randint(jax.random.fold_in(stream_key, axis), (), 0, length) for axis, length in enumerate(values.shape)]
    longest = values.shape.index(max(values.shape))
    next_to = spot[:longest] + [(spot[longest] + 1) % values.shape[longest]] + spot[longest + 1:]
    return values.at[tuple(spot)].set(low).at[tuple(next_to)].set(high)


def level_of(rng, shape, pieces, low, largest):
    factor_of = 1.0
    for position, blocks in pieces:
        draws = jax.random.uniform(jax.random.fold_in(jax.random.fold_in(rng, 6), position), (blocks,), jnp.float32, low / len(pieces), largest / len(pieces))
        factor_of = factor_of * jnp.repeat(jnp.exp(draws), shape[position] // blocks).reshape((-1,) + (1,) * (len(shape) - 1 - position))
    return factor_of


def scatter_about(key, extent, deviation, most, split=(), kind=jnp.bfloat16):
    entries = jax.random.normal(key, extent, jnp.float32) * deviation
    if len(split) > 0:
        entries = level_of(key, extent, split, -0.22, 0.18) * entries
    return jnp.clip(entries, min=-most, max=most).astype(kind)


def setup_inputs(seed: int = 0) -> dict:
    key_list = jax.random.split(jax.random.key(seed), 5)
    return {
        "object_field": scatter_about(key_list[0], (2, NR, NC), 1.0, 6.0, ((1, 4), (2, 32)), jnp.float32),
        "probe": scatter_about(key_list[1], (2, WIN, WIN), 1.0, 6.0, (), jnp.float32),
        "amplitudes": jnp.clip(jnp.exp(math.log(4.0) - 2.0794415 * jax.random.uniform(key_list[2], (TR, TC, POS, WIN, WIN), jnp.float32) ** level_of(key_list[2], (TR, TC, POS, WIN, WIN), ((0, 4), (1, 32)), -0.2, 0.2)), 0.5, 4.0),
        "offsets": set_ends(jax.random.randint(key_list[3], (TR, TC, POS, 2), 0, 3 * OWN - WIN + 1), jax.random.fold_in(key_list[3], 1), 0, 3 * OWN - WIN).astype(jnp.int32),
    }


floor_level = 0.5

def window_term(window, probe, amp):
    pr, pi = (probe[0], probe[1])
    orr, oi = (window[0], window[1])
    er = pr * orr - pi * oi
    ei = pr * oi + pi * orr
    far = jnp.fft.fft2(er + 1j * ei, norm='ortho')
    fr = jnp.real(far)
    fi = jnp.imag(far)
    modulus = jnp.sqrt(fr * fr + fi * fi)
    keep = 1.0 - amp / jnp.maximum(modulus, floor_level)
    back = jnp.fft.ifft2(fr * keep + 1j * (fi * keep), norm='ortho')
    br = jnp.real(back)
    bi = jnp.imag(back)
    return jnp.stack([pr * br + pi * bi, pr * bi - pi * br])

def reference(object_field, probe, amplitudes, offsets):
    count = TR * TC * POS
    index = jnp.arange(count, dtype=jnp.int32)
    tile_row = index // (TC * POS)
    tile_col = index // POS % TC
    starts = offsets.reshape(count, 2).astype(jnp.int32)
    first = tile_row * OWN + starts[:, 0]
    second = tile_col * OWN + starts[:, 1]
    amps = amplitudes.reshape(count, WIN, WIN)
    zero = jnp.zeros((), jnp.int32)
    power = (probe[0] * probe[0] + probe[1] * probe[1])[None]

    def light_step(acc, item):
        y0, x0 = item
        cur = lax.dynamic_slice(acc, (zero, y0, x0), (1, WIN, WIN))
        return (lax.dynamic_update_slice(acc, cur + power, (zero, y0, x0)), None)
    light = jnp.zeros((1, NR + 2 * OWN, NC + 2 * OWN), jnp.float32)
    light, _ = lax.scan(light_step, light, (first, second))
    illumination = light[:, OWN:OWN + NR, OWN:OWN + NC]
    field = object_field
    for step in range(ITERS):
        padded = jnp.pad(field, ((0, 0), (OWN, OWN), (OWN, OWN)))

        def grad_step(acc, item):
            y0, x0, amp = item
            window = lax.dynamic_slice(padded, (zero, y0, x0), (2, WIN, WIN))
            term = window_term(window, probe, amp)
            cur = lax.dynamic_slice(acc, (zero, y0, x0), (2, WIN, WIN))
            return (lax.dynamic_update_slice(acc, cur + term, (zero, y0, x0)), None)
        acc = jnp.zeros((2, NR + 2 * OWN, NC + 2 * OWN), jnp.float32)
        acc, _ = lax.scan(grad_step, acc, (first, second, amps))
        gradient = acc[:, OWN:OWN + NR, OWN:OWN + NC]
        field = field - gradient / (illumination + 1.0)
    return field
```

```python
import functools
import math

import jax
import jax.numpy as jnp
import numpy as np
from jax import lax
from jax.experimental import pallas as pl
from jax.experimental.pallas import tpu as pltpu
from jax.sharding import PartitionSpec as P

ITERS = 2
T = 128
W = 256
MESH = pl.DeviceIdType.MESH
f32 = jnp.float32
bf16 = jnp.bfloat16


def dft_parts():
    m = np.arange(T)
    mats = []
    for odd in (0, 1):
        turns = (m[:, None] * (2 * m[None, :] + odd)) % W
        angle = 2.0 * np.pi / W * turns
        c, s = np.cos(angle) / 16.0, np.sin(angle) / 16.0
        mats.append(np.block([[c, -s], [s, c]]))
    mats = [mats[0], mats[1], mats[0].T, mats[1].T]
    out = []
    for a in mats:
        a = a.astype(np.float32)
        hi = a.astype(jnp.bfloat16)
        lo = (a - hi.astype(np.float32)).astype(jnp.bfloat16)
        out += [hi, lo]
    return np.stack(out)


def split(x):
    hi = x.astype(bf16)
    return hi, (x - hi.astype(f32)).astype(bf16)


def mm(a, b):
    return jnp.dot(a, b, preferred_element_type=f32)


def kernel(
    n_rows, n_cols, n_pos,
    obj_ref, off_ref, probe_hbm, amp_hbm, mats_hbm,
    out_ref,
    G, A, FC, FX, FY, ill, probe, amp, mats, rolled, ampp, halves,
    g_send, g_recv, f_send, f_recv, l_sem,
):
    r = lax.axis_index("rows")
    c = lax.axis_index("cols")
    ro, h = lax.rem(r, 2), lax.rem(c, 2)
    rc, rx = r + 1 - 2 * ro, r - 1 + 2 * ro
    cp = c + 1 - 2 * h
    cx, cf = c + 2 - 4 * h, c - 2 + 4 * h
    has_x = (rx >= 0) & (rx < n_rows)
    has_cx = (cx >= 0) & (cx < n_cols)
    has_far = (cf >= 0) & (cf < n_cols)
    rcs = rc - r + 1
    rxs = 2 - rcs
    hp = cp - c + 1
    fp = 2 - hp

    local = [
        pltpu.make_async_copy(probe_hbm, probe, l_sem.at[0]),
        pltpu.make_async_copy(amp_hbm, amp, l_sem.at[1]),
        pltpu.make_async_copy(mats_hbm, mats, l_sem.at[2]),
    ]
    for copy in local:
        copy.start()

    barrier = pltpu.get_barrier_semaphore()

    def greet(row, col):
        pl.semaphore_signal(
            barrier, inc=1, device_id={"rows": row, "cols": col}, device_id_type=MESH
        )

    greet(rc, c)
    greet(r, cp)

    @pl.when(has_x)
    def _():
        greet(rx, c)
        greet(rx, cp)

    @pl.when(has_cx)
    def _():
        greet(r, cx)

    @pl.when(has_far)
    def _():
        greet(r, cf)

    always = None

    def both(a, b):
        return a & b

    def when(cond, f):
        if cond is None:
            f()
        else:
            pl.when(cond)(f)

    g_sends = {2: has_x, 3: has_x, 4: has_cx, 5: both(has_x, has_cx), 7: has_far}
    g_recvs = {2: has_x, 3: has_x, 4: has_far, 5: both(has_x, has_far), 7: has_far}

    def g_copy(L, k):
        src, dst, dev = {
            0: ((1, 1), (2 - rcs, 1), (rc, c)),
            1: ((1, 1), (1, 2 - hp), (r, cp)),
            2: ((1, 1), (2 - rxs, 1), (rx, c)),
            3: ((1, 1), (2 - rxs, 2 - hp), (rx, cp)),
            4: ((1, hp), (1, fp), (r, cx)),
            5: ((rxs, hp), (rxs, fp), (r, cx)),
            6: ((1, hp), (2 - rcs, hp), (rc, c)),
            7: ((1, fp), (2 - rcs, fp), (rc, c)),
        }[k]
        return pltpu.make_async_remote_copy(
            src_ref=G.at[(L,) + src],
            dst_ref=G.at[(L,) + dst],
            send_sem=g_send.at[L, k],
            recv_sem=g_recv.at[L, k],
            device_id={"rows": dev[0], "cols": dev[1]},
            device_id_type=MESH,
        )

    def g_start(L, k):
        when(g_sends.get(k, always), lambda: g_copy(L, k).start())

    def g_wait(L, k):
        when(g_recvs.get(k, always), lambda: g_copy(L, k).wait_recv())

    def g_begin(planes):
        for L in planes:
            for k in (1, 3, 2, 0):
                g_start(L, k)

    def g_finish(planes):
        for L in planes:
            g_wait(L, 1)
            g_start(L, 4)
            g_start(L, 6)
            g_wait(L, 3)
            g_start(L, 5)
        for L in planes:
            g_wait(L, 4)
            g_start(L, 7)
        for L in planes:
            for k in (0, 2, 5, 6, 7):
                g_wait(L, k)

    f_sends = {1: has_far, 2: both(has_x, has_far), 4: has_x, 5: has_x}
    f_recvs = {1: has_cx, 2: both(has_x, has_cx), 4: has_x, 5: has_x}

    def f_copy(L, k):
        src, dst, dev = {
            0: (A.at[L, rcs], FC.at[L], (rc, c)),
            1: (A.at[L, 1, fp], FX.at[L, 0], (r, cf)),
            2: (A.at[L, rxs, fp], FX.at[L, 1], (r, cf)),
            3: (A.at[L, 1, hp], FY.at[L, 0], (r, cp)),
            4: (A.at[L, rxs, 1], FY.at[L, 1], (rx, c)),
            5: (A.at[L, rxs, hp], FY.at[L, 2], (rx, cp)),
        }[k]
        return pltpu.make_async_remote_copy(
            src_ref=src,
            dst_ref=dst,
            send_sem=f_send.at[L, k],
            recv_sem=f_recv.at[L, k],
            device_id={"rows": dev[0], "cols": dev[1]},
            device_id_type=MESH,
        )

    def f_start(L, k):
        when(f_sends.get(k, always), lambda: f_copy(L, k).start())

    def f_wait(L, k):
        when(f_recvs.get(k, always), lambda: f_copy(L, k).wait_recv())

    def f_begin(planes):
        for L in planes:
            for k in (0, 2, 4):
                f_start(L, k)

    def f_core(planes):
        for L in planes:
            f_wait(L, 0)
            A[L, 1, fp] += FC[L, fp]
            f_start(L, 1)
        for L in planes:
            A[L, 1, hp] += FC[L, hp]

    def f_across(planes):
        for L in planes:
            f_wait(L, 2)

            @pl.when(f_recvs[2])
            def _():
                A[L, rxs, hp] += FX[L, 1]

            f_start(L, 5)
            f_wait(L, 1)

            @pl.when(has_cx)
            def _():
                A[L, 1, hp] += FX[L, 0]

            f_start(L, 3)

    def f_end(L):
        f_wait(L, 3)
        f_wait(L, 4)
        f_wait(L, 5)
        return A[L, 1, 1] + FC[L, 1] + FY[L, 0] + FY[L, 1] + FY[L, 2]

    for plane in range(2):
        G[plane, 1, 1] = obj_ref[plane]
    greeted = 2 + 2 * has_x.astype(jnp.int32) + has_cx.astype(jnp.int32) + has_far.astype(jnp.int32)
    pl.semaphore_wait(barrier, greeted)
    g_begin((0, 1))

    zero_tile = jnp.zeros((T, T), f32)

    @pl.when(jnp.logical_not(has_x))
    def _():
        for L in range(2 * ITERS):
            for col in range(3):
                G[L, rxs, col] = zero_tile
        for L in range(2 * ITERS + 1):
            FY[L, 1] = zero_tile
            FY[L, 2] = zero_tile

    @pl.when(jnp.logical_not(has_far))
    def _():
        for L in range(2 * ITERS):
            for row in range(3):
                G[L, row, fp] = zero_tile

    for L in range(2 * ITERS + 1):
        for row in range(3):
            for col in range(3):
                A[L, row, col] = zero_tile

    row_of = lax.broadcasted_iota(jnp.int32, (T, T), 0)
    col_of = lax.broadcasted_iota(jnp.int32, (T, T), 1)

    def add_term(L, p, term):
        mr = row_of >= off_ref[p, 0]
        mc = col_of >= off_ref[p, 1]
        zero = jnp.zeros((T, T), f32)
        top = jnp.where(mr, term[0][0], zero)
        low = term[0][0] - top
        A[L, 0, 0] += jnp.where(mc, top, zero)
        A[L, 0, 2] += jnp.where(mc, zero, top)
        A[L, 2, 0] += jnp.where(mc, low, zero)
        A[L, 2, 2] += jnp.where(mc, zero, low)
        A[L, 0, 1] += jnp.where(mr, term[0][1], zero)
        A[L, 2, 1] += jnp.where(mr, zero, term[0][1])
        A[L, 1, 0] += jnp.where(mc, term[1][0], zero)
        A[L, 1, 2] += jnp.where(mc, zero, term[1][0])
        A[L, 1, 1] += term[1][1]

    def blocks(x):
        return [[x[i * T:(i + 1) * T, j * T:(j + 1) * T] for j in range(2)] for i in range(2)]

    local[0].wait()

    def roll_probe(p, carry):
        power = None
        for plane in range(2):
            x = pltpu.roll(probe[plane], off_ref[p, 0], 0)
            x = pltpu.roll(x, off_ref[p, 1], 1)
            rolled[p, plane] = x
            power = x * x if power is None else power + x * x
        add_term(2 * ITERS, p, blocks(power))
        return carry

    lax.fori_loop(0, n_pos, roll_probe, 0)

    local[1].wait()
    lane_in = lax.broadcasted_iota(jnp.int32, (W, W), 0)
    lane_out = lax.broadcasted_iota(jnp.int32, (W, W), 1)
    source = jnp.where(lane_out < T, 2 * lane_out, 2 * lane_out - (W - 1))
    perm = jnp.where(lane_in == source, 1.0, 0.0).astype(bf16)

    def permute_amp(p, carry):
        x = amp[p]
        hi = x.astype(bf16)
        mid, low = split(x - hi.astype(f32))
        x = mm(hi, perm) + mm(mid, perm) + mm(low, perm)
        for half in range(2):
            lanes = pl.ds(half * T, T)
            halves[half] = x[:, half * T:(half + 1) * T]
            for par in range(2):
                ampp[p, par, :, lanes] = halves[half, pl.ds(par, T, stride=2), :]
        return carry

    lax.fori_loop(0, n_pos, permute_amp, 0)
    local[2].wait()

    def right(x, m):
        hi, lo = split(x)
        return mm(hi, mats[m]) + mm(lo, mats[m]) + mm(hi, mats[m + 1])

    def left(m, x):
        hi, lo = split(x)
        return mm(mats[m], hi) + mm(mats[m + 1], hi) + mm(mats[m], lo)

    def window(it, p):
        mr = row_of >= off_ref[p, 0]
        mc = col_of >= off_ref[p, 1]
        ob = []
        for L in (2 * it, 2 * it + 1):
            t = lambda a, b: G[L, a, b]
            ob.append([
                [
                    jnp.where(mr, jnp.where(mc, t(0, 0), t(0, 2)), jnp.where(mc, t(2, 0), t(2, 2))),
                    jnp.where(mr, t(0, 1), t(2, 1)),
                ],
                [jnp.where(mc, t(1, 0), t(1, 2)), t(1, 1)],
            ])
        pr = blocks(rolled[p, 0])
        pi = blocks(rolled[p, 1])
        us, vs = [], []
        for i in range(2):
            er = [pr[i][j] * ob[0][i][j] - pi[i][j] * ob[1][i][j] for j in range(2)]
            ei = [pr[i][j] * ob[1][i][j] + pi[i][j] * ob[0][i][j] for j in range(2)]
            us.append(jnp.concatenate([er[0] + er[1], ei[0] + ei[1]], 1))
            vs.append(jnp.concatenate([er[0] - er[1], ei[0] - ei[1]], 1))
        even = right(jnp.concatenate(us, 0), 0)
        odd = right(jnp.concatenate(vs, 0), 2)
        yr = jnp.concatenate([even[:, :T], odd[:, :T]], 1)
        yi = jnp.concatenate([even[:, T:], odd[:, T:]], 1)
        u = jnp.concatenate([yr[:T] + yr[T:], yi[:T] + yi[T:]], 0)
        v = jnp.concatenate([yr[:T] - yr[T:], yi[:T] - yi[T:]], 0)
        back = []
        for par, x in ((0, u), (1, v)):
            far = left(4 + 2 * par, x)
            fr, fi = far[:T], far[T:]
            keep = 1.0 - ampp[p, par] * lax.rsqrt(jnp.maximum(fr * fr + fi * fi, 0.25))
            back.append(left(2 * par, jnp.concatenate([fr * keep, fi * keep], 0)))
        tot, dif = back[0] + back[1], back[0] - back[1]
        zr = jnp.concatenate([tot[:T], dif[:T]], 0)
        zi = jnp.concatenate([tot[T:], dif[T:]], 0)
        even = right(jnp.concatenate([zr[:, :T], zi[:, :T]], 1), 4)
        odd = right(jnp.concatenate([zr[:, T:], zi[:, T:]], 1), 6)
        tot, dif = even + odd, even - odd
        tr, ti = [], []
        for i in range(2):
            rows = slice(i * T, (i + 1) * T)
            br = [tot[rows, :T], dif[rows, :T]]
            bi = [tot[rows, T:], dif[rows, T:]]
            tr.append([pr[i][j] * br[j] + pi[i][j] * bi[j] for j in range(2)])
            ti.append([pr[i][j] * bi[j] - pi[i][j] * br[j] for j in range(2)])
        add_term(2 * it, p, tr)
        add_term(2 * it + 1, p, ti)

    def windows(it, first, last):
        def step(p, carry):
            window(it, p)
            return carry

        lax.fori_loop(first, last, step, 0)

    g_finish((0, 1))
    light = (2 * ITERS,)
    f_begin(light)
    for it in range(ITERS):
        if it == 0:
            half = n_pos // 2
            windows(it, 0, half)
            f_core(light)
            windows(it, half, n_pos)
        else:
            windows(it, 0, n_pos)
        planes = (2 * it, 2 * it + 1)
        f_begin(planes)
        if it == 0:
            f_across(light)
        f_core(planes)
        f_across(planes)
        if it == 0:
            ill[...] = f_end(2 * ITERS) + 1.0
        for plane in range(2):
            L = 2 * it + plane
            new = G[L, 1, 1] - f_end(L) / ill[...]
            if it < ITERS - 1:
                G[L + 2, 1, 1] = new
                g_begin((L + 2,))
            else:
                out_ref[plane] = new
        if it < ITERS - 1:
            g_finish((2 * it + 2, 2 * it + 3))

    for L in range(2 * ITERS):
        for k in range(8):
            when(g_sends.get(k, always), lambda L=L, k=k: g_copy(L, k).wait_send())
    for L in range(2 * ITERS + 1):
        for k in range(6):
            when(f_sends.get(k, always), lambda L=L, k=k: f_copy(L, k).wait_send())


def local(n_rows, n_cols, object_field, probe, amplitudes, offsets):
    n_pos = amplitudes.shape[2]
    n = 2 * ITERS
    anyspace = pl.BlockSpec(memory_space=pl.ANY)
    vmem = pl.BlockSpec(memory_space=pltpu.VMEM)
    return pl.pallas_call(
        functools.partial(kernel, n_rows, n_cols, n_pos),
        out_shape=jax.ShapeDtypeStruct(object_field.shape, f32),
        in_specs=[vmem, pl.BlockSpec(memory_space=pltpu.SMEM), anyspace, anyspace, anyspace],
        out_specs=vmem,
        scratch_shapes=[
            pltpu.VMEM((n, 3, 3, T, T), f32),
            pltpu.VMEM((n + 1, 3, 3, T, T), f32),
            pltpu.VMEM((n + 1, 3, T, T), f32),
            pltpu.VMEM((n + 1, 2, T, T), f32),
            pltpu.VMEM((n + 1, 3, T, T), f32),
            pltpu.VMEM((T, T), f32),
            pltpu.VMEM((2, W, W), f32),
            pltpu.VMEM((n_pos, W, W), f32),
            pltpu.VMEM((8, W, W), bf16),
            pltpu.VMEM((n_pos, 2, W, W), f32),
            pltpu.VMEM((n_pos, 2, T, W), f32),
            pltpu.VMEM((2, W, T), f32),
            pltpu.SemaphoreType.DMA((n, 8)),
            pltpu.SemaphoreType.DMA((n, 8)),
            pltpu.SemaphoreType.DMA((n + 1, 6)),
            pltpu.SemaphoreType.DMA((n + 1, 6)),
            pltpu.SemaphoreType.DMA((3,)),
        ],
        compiler_params=pltpu.CompilerParams(
            collective_id=0, has_side_effects=True, vmem_limit_bytes=56 * 1024 * 1024
        ),
    )(
        object_field,
        offsets[0, 0],
        probe,
        amplitudes[0, 0],
        jnp.asarray(dft_parts()),
    )


def solution(mesh):
    placed = (
        P(None, "rows", "cols"),
        P(),
        P("rows", "cols", None, None, None),
        P("rows", "cols", None, None),
    )
    body = functools.partial(local, mesh.shape["rows"], mesh.shape["cols"])
    return jax.shard_map(
        body, mesh=mesh, in_specs=placed, out_specs=P(None, "rows", "cols"), check_vma=False
    )
```

```python
import functools
import math

import jax
import jax.numpy as jnp
import numpy as np
from jax import lax
from jax.experimental import pallas as pl
from jax.experimental.pallas import tpu as pltpu
from jax.sharding import PartitionSpec as P

ITERS = 2
T = 128
W = 256
CHUNK = 64
GROUP = 2
VMEM_MIB = 28
MESH = pl.DeviceIdType.MESH
f32 = jnp.float32
bf16 = jnp.bfloat16


def dft_parts():
    m = np.arange(T)
    mats = []
    for odd in (0, 1):
        turns = (m[:, None] * (2 * m[None, :] + odd)) % W
        angle = 2.0 * np.pi / W * turns
        c, s = np.cos(angle) / 16.0, np.sin(angle) / 16.0
        mats.append(np.block([[c, -s], [s, c]]))
    mats = [mats[0], mats[1], mats[0].T, mats[1].T]
    out = []
    for a in mats:
        a = a.astype(np.float32)
        hi = a.astype(jnp.bfloat16)
        lo = (a - hi.astype(np.float32)).astype(jnp.bfloat16)
        out += [hi, lo]
    return np.stack(out)


def split(x):
    hi = x.astype(bf16)
    return hi, (x - hi.astype(f32)).astype(bf16)


def mm(a, b):
    return jnp.dot(a, b, preferred_element_type=f32)


def kernel(
    n_rows, n_cols, n_pos,
    obj_hbm, off_ref, probe_hbm, amp_hbm, mats_hbm,
    out_ref,
    G, A, FC, FX, FY, ill, probe, amp, mats, rolled, ampp, halves,
    g_send, g_recv, f_send, f_recv, l_sem,
):
    r = lax.axis_index("rows")
    c = lax.axis_index("cols")
    ro, h = lax.rem(r, 2), lax.rem(c, 2)
    rc, rx = r + 1 - 2 * ro, r - 1 + 2 * ro
    cp = c + 1 - 2 * h
    cx, cf = c + 2 - 4 * h, c - 2 + 4 * h
    has_x = (rx >= 0) & (rx < n_rows)
    has_cx = (cx >= 0) & (cx < n_cols)
    has_far = (cf >= 0) & (cf < n_cols)
    rcs = rc - r + 1
    rxs = 2 - rcs
    hp = cp - c + 1
    fp = 2 - hp

    local = [
        pltpu.make_async_copy(probe_hbm, probe, l_sem.at[0]),
        pltpu.make_async_copy(amp_hbm, amp, l_sem.at[1]),
        pltpu.make_async_copy(mats_hbm, mats, l_sem.at[2]),
        pltpu.make_async_copy(obj_hbm.at[0], G.at[0, 1, 1], l_sem.at[3]),
        pltpu.make_async_copy(obj_hbm.at[1], G.at[1, 1, 1], l_sem.at[4]),
    ]
    for i in (3, 4, 0, 1, 2):
        local[i].start()

    barrier = pltpu.get_barrier_semaphore()

    def greet(row, col):
        pl.semaphore_signal(
            barrier, inc=1, device_id={"rows": row, "cols": col}, device_id_type=MESH
        )

    greet(rc, c)
    greet(r, cp)

    @pl.when(has_x)
    def _():
        greet(rx, c)
        greet(rx, cp)

    @pl.when(has_cx)
    def _():
        greet(r, cx)

    @pl.when(has_far)
    def _():
        greet(r, cf)

    always = None

    def both(a, b):
        return a & b

    def when(cond, f):
        if cond is None:
            f()
        else:
            pl.when(cond)(f)

    g_sends = {2: has_x, 3: has_x, 4: has_cx, 5: both(has_x, has_cx), 7: has_far}
    g_recvs = {2: has_x, 3: has_x, 4: has_far, 5: both(has_x, has_far), 7: has_far}

    def g_copy(L, k, q):
        src, dst, dev = {
            0: ((1, 1), (2 - rcs, 1), (rc, c)),
            1: ((1, 1), (1, 2 - hp), (r, cp)),
            2: ((1, 1), (2 - rxs, 1), (rx, c)),
            3: ((1, 1), (2 - rxs, 2 - hp), (rx, cp)),
            4: ((1, hp), (1, fp), (r, cx)),
            5: ((rxs, hp), (rxs, fp), (r, cx)),
            6: ((1, hp), (2 - rcs, hp), (rc, c)),
            7: ((1, fp), (2 - rcs, fp), (rc, c)),
        }[k]
        part = (pl.ds(q * CHUNK, CHUNK),)
        return pltpu.make_async_remote_copy(
            src_ref=G.at[(L,) + src + part],
            dst_ref=G.at[(L,) + dst + part],
            send_sem=g_send.at[L, k, q],
            recv_sem=g_recv.at[L, k, q],
            device_id={"rows": dev[0], "cols": dev[1]},
            device_id_type=MESH,
        )

    def g_start(L, k, q):
        when(g_sends.get(k, always), lambda: g_copy(L, k, q).start())

    def g_wait(L, k, q):
        when(g_recvs.get(k, always), lambda: g_copy(L, k, q).wait_recv())

    def chunks(planes):
        return [(L, q) for L in planes for q in range(T // CHUNK)]

    def g_begin(planes, kinds):
        for k in kinds:
            for L, q in chunks(planes):
                g_start(L, k, q)

    def g_finish(planes):
        for L, q in chunks(planes):
            g_wait(L, 1, q)
            g_start(L, 4, q)
            g_start(L, 6, q)
        for L, q in chunks(planes):
            g_wait(L, 3, q)
            g_start(L, 5, q)
        for L, q in chunks(planes):
            g_wait(L, 4, q)
            g_start(L, 7, q)
        for k in (0, 2, 5, 6, 7):
            for L, q in chunks(planes):
                g_wait(L, k, q)

    f_sends = {1: has_far, 2: both(has_x, has_far), 4: has_x, 5: has_x}
    f_recvs = {1: has_cx, 2: both(has_x, has_cx), 4: has_x, 5: has_x}

    def f_copy(L, k, q):
        part = pl.ds(q * CHUNK, CHUNK)
        src, dst, dev = {
            0: (A.at[L, rcs, fp, part], FC.at[L, fp, part], (rc, c)),
            1: (A.at[L, 1, fp, part], FX.at[L, 0, part], (r, cf)),
            2: (A.at[L, rxs, fp, part], FX.at[L, 1, part], (r, cf)),
            3: (A.at[L, 1, hp, part], FY.at[L, 0, part], (r, cp)),
            4: (A.at[L, rxs, 1, part], FY.at[L, 1, part], (rx, c)),
            5: (A.at[L, rxs, hp, part], FY.at[L, 2, part], (rx, cp)),
            6: (A.at[L, rcs, hp, part], FC.at[L, hp, part], (rc, c)),
            7: (A.at[L, rcs, 1, part], FC.at[L, 1, part], (rc, c)),
        }[k]
        return pltpu.make_async_remote_copy(
            src_ref=src,
            dst_ref=dst,
            send_sem=f_send.at[L, k, q],
            recv_sem=f_recv.at[L, k, q],
            device_id={"rows": dev[0], "cols": dev[1]},
            device_id_type=MESH,
        )

    def f_start(L, k, q):
        when(f_sends.get(k, always), lambda: f_copy(L, k, q).start())

    def f_wait(L, k, q):
        when(f_recvs.get(k, always), lambda: f_copy(L, k, q).wait_recv())

    def f_begin(planes, kinds=(0, 4, 2, 6, 7)):
        for k in kinds:
            for L, q in chunks(planes):
                f_start(L, k, q)

    def f_core(planes, send=True):
        for L, q in chunks(planes):
            part = pl.ds(q * CHUNK, CHUNK)
            f_wait(L, 0, q)
            A[L, 1, fp, part] += FC[L, fp, part]
            if send:
                f_start(L, 1, q)
        for L, q in chunks(planes):
            part = pl.ds(q * CHUNK, CHUNK)
            f_wait(L, 6, q)
            A[L, 1, hp, part] += FC[L, hp, part]

    def f_across(planes):
        for L, q in chunks(planes):
            part = pl.ds(q * CHUNK, CHUNK)
            f_wait(L, 2, q)

            @pl.when(f_recvs[2])
            def _():
                A[L, rxs, hp, part] += FX[L, 1, part]

            f_start(L, 5, q)
        for L, q in chunks(planes):
            part = pl.ds(q * CHUNK, CHUNK)
            f_wait(L, 1, q)

            @pl.when(has_cx)
            def _():
                A[L, 1, hp, part] += FX[L, 0, part]

            f_start(L, 3, q)

    def f_end(L, q):
        part = pl.ds(q * CHUNK, CHUNK)
        for k in (7, 4, 5, 3):
            f_wait(L, k, q)
        return A[L, 1, 1, part] + FC[L, 1, part] + FY[L, 0, part] + FY[L, 1, part] + FY[L, 2, part]

    local[3].wait()
    local[4].wait()
    greeted = 2 + 2 * has_x.astype(jnp.int32) + has_cx.astype(jnp.int32) + has_far.astype(jnp.int32)
    pl.semaphore_wait(barrier, greeted)
    g_begin((0, 1), (1, 2, 3, 0))

    zero_tile = jnp.zeros((T, T), f32)

    @pl.when(jnp.logical_not(has_x))
    def _():
        for L in range(2 * ITERS):
            for col in range(3):
                G[L, rxs, col] = zero_tile
        for L in range(2 * ITERS + 1):
            FY[L, 1] = zero_tile
            FY[L, 2] = zero_tile

    @pl.when(jnp.logical_not(has_far))
    def _():
        for L in range(2 * ITERS):
            for row in range(3):
                G[L, row, fp] = zero_tile

    for L in range(2 * ITERS + 1):
        for row in range(3):
            for col in range(3):
                A[L, row, col] = zero_tile

    row_of = lax.broadcasted_iota(jnp.int32, (T, T), 0)
    col_of = lax.broadcasted_iota(jnp.int32, (T, T), 1)

    def add_term(L, p, term):
        mr = row_of >= off_ref[0, p]
        mc = col_of >= off_ref[1, p]
        zero = jnp.zeros((T, T), f32)
        top = jnp.where(mr, term[0][0], zero)
        low = term[0][0] - top
        A[L, 0, 0] += jnp.where(mc, top, zero)
        A[L, 0, 2] += jnp.where(mc, zero, top)
        A[L, 2, 0] += jnp.where(mc, low, zero)
        A[L, 2, 2] += jnp.where(mc, zero, low)
        A[L, 0, 1] += jnp.where(mr, term[0][1], zero)
        A[L, 2, 1] += jnp.where(mr, zero, term[0][1])
        A[L, 1, 0] += jnp.where(mc, term[1][0], zero)
        A[L, 1, 2] += jnp.where(mc, zero, term[1][0])
        A[L, 1, 1] += term[1][1]

    def blocks(x):
        return [[x[i * T:(i + 1) * T, j * T:(j + 1) * T] for j in range(2)] for i in range(2)]

    local[0].wait()

    def roll_probe(p, carry):
        power = None
        for plane in range(2):
            x = pltpu.roll(probe[plane], off_ref[0, p], 0)
            x = pltpu.roll(x, off_ref[1, p], 1)
            rolled[p, plane] = x
            power = x * x if power is None else power + x * x
        add_term(2 * ITERS, p, blocks(power))
        return carry

    lax.fori_loop(0, n_pos, roll_probe, 0)
    light = (2 * ITERS,)
    f_begin(light, (0, 6, 7))

    local[1].wait()
    lane_in = lax.broadcasted_iota(jnp.int32, (W, W), 0)
    lane_out = lax.broadcasted_iota(jnp.int32, (W, W), 1)
    source = jnp.where(lane_out < T, 2 * lane_out, 2 * lane_out - (W - 1))
    perm = jnp.where(lane_in == source, 1.0, 0.0).astype(bf16)

    def permute_amp(p, carry):
        x = amp[p]
        hi = x.astype(bf16)
        mid, low = split(x - hi.astype(f32))
        x = mm(hi, perm) + mm(mid, perm) + mm(low, perm)
        for half in range(2):
            lanes = pl.ds(half * T, T)
            halves[half] = x[:, half * T:(half + 1) * T]
            for par in range(2):
                ampp[p, par, :, lanes] = halves[half, pl.ds(par, T, stride=2), :]
        return carry

    lax.fori_loop(0, n_pos, permute_amp, 0)
    local[2].wait()

    def right(x, m):
        hi, lo = split(x)
        return mm(hi, mats[m]) + mm(lo, mats[m]) + mm(hi, mats[m + 1])

    def left(m, x):
        hi, lo = split(x)
        return mm(mats[m], hi) + mm(mats[m + 1], hi) + mm(mats[m], lo)

    def window(it, p):
        mr = row_of >= off_ref[0, p]
        mc = col_of >= off_ref[1, p]
        ob = []
        for L in (2 * it, 2 * it + 1):
            t = lambda a, b: G[L, a, b]
            ob.append([
                [
                    jnp.where(mr, jnp.where(mc, t(0, 0), t(0, 2)), jnp.where(mc, t(2, 0), t(2, 2))),
                    jnp.where(mr, t(0, 1), t(2, 1)),
                ],
                [jnp.where(mc, t(1, 0), t(1, 2)), t(1, 1)],
            ])
        pr = blocks(rolled[p, 0])
        pi = blocks(rolled[p, 1])
        us, vs = [], []
        for i in range(2):
            er = [pr[i][j] * ob[0][i][j] - pi[i][j] * ob[1][i][j] for j in range(2)]
            ei = [pr[i][j] * ob[1][i][j] + pi[i][j] * ob[0][i][j] for j in range(2)]
            us.append(jnp.concatenate([er[0] + er[1], ei[0] + ei[1]], 1))
            vs.append(jnp.concatenate([er[0] - er[1], ei[0] - ei[1]], 1))
        even = right(jnp.concatenate(us, 0), 0)
        odd = right(jnp.concatenate(vs, 0), 2)
        yield
        yr = jnp.concatenate([even[:, :T], odd[:, :T]], 1)
        yi = jnp.concatenate([even[:, T:], odd[:, T:]], 1)
        u = jnp.concatenate([yr[:T] + yr[T:], yi[:T] + yi[T:]], 0)
        v = jnp.concatenate([yr[:T] - yr[T:], yi[:T] - yi[T:]], 0)
        back = []
        fars = [left(4 + 2 * par, x) for par, x in ((0, u), (1, v))]
        yield
        for par, far in enumerate(fars):
            fr, fi = far[:T], far[T:]
            keep = 1.0 - ampp[p, par] * lax.rsqrt(jnp.maximum(fr * fr + fi * fi, 0.25))
            back.append(left(2 * par, jnp.concatenate([fr * keep, fi * keep], 0)))
        yield
        tot, dif = back[0] + back[1], back[0] - back[1]
        zr = jnp.concatenate([tot[:T], dif[:T]], 0)
        zi = jnp.concatenate([tot[T:], dif[T:]], 0)
        even = right(jnp.concatenate([zr[:, :T], zi[:, :T]], 1), 4)
        odd = right(jnp.concatenate([zr[:, T:], zi[:, T:]], 1), 6)
        yield
        tot, dif = even + odd, even - odd
        tr, ti = [], []
        for i in range(2):
            rows = slice(i * T, (i + 1) * T)
            br = [tot[rows, :T], dif[rows, :T]]
            bi = [tot[rows, T:], dif[rows, T:]]
            tr.append([pr[i][j] * br[j] + pi[i][j] * bi[j] for j in range(2)])
            ti.append([pr[i][j] * bi[j] - pi[i][j] * br[j] for j in range(2)])
        add_term(2 * it, p, tr)
        add_term(2 * it + 1, p, ti)
        yield

    def windows(it, first, last):
        def step(t, carry):
            running = [window(it, first + GROUP * t + i) for i in range(GROUP)]
            for _ in range(5):
                for one in running:
                    next(one)
            return carry

        lax.fori_loop(0, (last - first) // GROUP, step, 0)

    g_finish((0, 1))
    f_core(light, False)
    f_begin(light, (4, 2, 1))
    for it in range(ITERS):
        planes = (2 * it, 2 * it + 1)
        if it == 0:
            half = n_pos // 2
            windows(it, 0, half)
            f_across(light)
            windows(it, half, n_pos)
        else:
            windows(it, 0, n_pos)
        f_begin(planes)
        if it == 0:
            for _, q in chunks(light):
                ill[pl.ds(q * CHUNK, CHUNK)] = f_end(2 * ITERS, q) + 1.0
        f_core(planes)
        f_across(planes)
        for L, q in chunks(planes):
            part = pl.ds(q * CHUNK, CHUNK)
            new = G[L, 1, 1, part] - f_end(L, q) / ill[part]
            if it < ITERS - 1:
                G[L + 2, 1, 1, part] = new
                g_start(L + 2, 1, q)
            else:
                out_ref[L - 2 * it, part] = new
        if it < ITERS - 1:
            planes = (2 * it + 2, 2 * it + 3)
            g_begin(planes, (2, 3, 0))
            g_finish(planes)

    for L, q in chunks(range(2 * ITERS)):
        for k in range(8):
            when(g_sends.get(k, always), lambda: g_copy(L, k, q).wait_send())
    for L, q in chunks(range(2 * ITERS + 1)):
        for k in range(8):
            when(f_sends.get(k, always), lambda: f_copy(L, k, q).wait_send())


def local(n_rows, n_cols, object_field, probe, amplitudes, offsets):
    n_pos = amplitudes.shape[2]
    n = 2 * ITERS

    def fix(x):
        return pltpu.with_memory_space_constraint(x, pltpu.HBM)

    hbm = pl.BlockSpec(memory_space=pltpu.HBM)
    vmem = pl.BlockSpec(memory_space=pltpu.VMEM)
    return pl.pallas_call(
        functools.partial(kernel, n_rows, n_cols, n_pos),
        out_shape=jax.ShapeDtypeStruct(object_field.shape, f32),
        in_specs=[hbm, pl.BlockSpec(memory_space=pltpu.SMEM), hbm, hbm, hbm],
        out_specs=vmem,
        scratch_shapes=[
            pltpu.VMEM((n, 3, 3, T, T), f32),
            pltpu.VMEM((n + 1, 3, 3, T, T), f32),
            pltpu.VMEM((n + 1, 3, T, T), f32),
            pltpu.VMEM((n + 1, 2, T, T), f32),
            pltpu.VMEM((n + 1, 3, T, T), f32),
            pltpu.VMEM((T, T), f32),
            pltpu.VMEM((2, W, W), f32),
            pltpu.VMEM((n_pos, W, W), f32),
            pltpu.VMEM((8, W, W), bf16),
            pltpu.VMEM((n_pos, 2, W, W), f32),
            pltpu.VMEM((n_pos, 2, T, W), f32),
            pltpu.VMEM((2, W, T), f32),
            pltpu.SemaphoreType.DMA((n, 8, T // CHUNK)),
            pltpu.SemaphoreType.DMA((n, 8, T // CHUNK)),
            pltpu.SemaphoreType.DMA((n + 1, 8, T // CHUNK)),
            pltpu.SemaphoreType.DMA((n + 1, 8, T // CHUNK)),
            pltpu.SemaphoreType.DMA((5,)),
        ],
        compiler_params=pltpu.CompilerParams(
            collective_id=0, has_side_effects=True, vmem_limit_bytes=VMEM_MIB * 1024 * 1024
        ),
    )(
        fix(object_field),
        fix(offsets[0, 0].T),
        fix(probe),
        fix(amplitudes[0, 0]),
        fix(jnp.asarray(dft_parts())),
    )


def solution(mesh):
    placed = (
        P(None, "rows", "cols"),
        P(),
        P("rows", "cols", None, None, None),
        P("rows", "cols", None, None),
    )
    body = functools.partial(local, mesh.shape["rows"], mesh.shape["cols"])
    return jax.shard_map(
        body, mesh=mesh, in_specs=placed, out_specs=P(None, "rows", "cols"), check_vma=False
    )
```

```python
import functools
import math

import jax
import jax.numpy as jnp
import numpy as np
from jax import lax
from jax.experimental import pallas as pl
from jax.experimental.pallas import tpu as pltpu
from jax.sharding import PartitionSpec as P

ITERS = 2
T = 128
W = 256
CHUNK = 64
GROUP = 2
VMEM_MIB = 28
MESH = pl.DeviceIdType.MESH
f32 = jnp.float32
bf16 = jnp.bfloat16


def dft_parts():
    m = np.arange(T)
    mats = []
    for odd in (0, 1):
        turns = (m[:, None] * (2 * m[None, :] + odd)) % W
        angle = 2.0 * np.pi / W * turns
        c, s = np.cos(angle) / 16.0, np.sin(angle) / 16.0
        mats.append(np.block([[c, -s], [s, c]]))
    mats = [mats[0], mats[1], mats[0].T, mats[1].T]
    out = []
    for a in mats:
        a = a.astype(np.float32)
        hi = a.astype(jnp.bfloat16)
        lo = (a - hi.astype(np.float32)).astype(jnp.bfloat16)
        out += [hi, lo]
    return np.stack(out)


def split(x):
    hi = x.astype(bf16)
    return hi, (x - hi.astype(f32)).astype(bf16)


def mm(a, b):
    return jnp.dot(a, b, preferred_element_type=f32)


def kernel(
    n_rows, n_cols, n_pos,
    obj_hbm, off_ref, probe_hbm, amp_hbm, mats_hbm,
    out_ref,
    G, A, FC, FR, FX, FY, ill, probe, amp, mats, rolled, ampp, halves, held,
    g_send, g_recv, f_send, f_recv, l_sem,
):
    r = lax.axis_index("rows")
    c = lax.axis_index("cols")
    ro, h = lax.rem(r, 2), lax.rem(c, 2)
    rc, rx = r + 1 - 2 * ro, r - 1 + 2 * ro
    cp = c + 1 - 2 * h
    cx, cf = c + 2 - 4 * h, c - 2 + 4 * h
    has_x = (rx >= 0) & (rx < n_rows)
    has_cx = (cx >= 0) & (cx < n_cols)
    has_far = (cf >= 0) & (cf < n_cols)
    rcs = rc - r + 1
    rxs = 2 - rcs
    hp = cp - c + 1
    fp = 2 - hp

    local = [
        pltpu.make_async_copy(probe_hbm, probe, l_sem.at[0]),
        pltpu.make_async_copy(amp_hbm, amp, l_sem.at[1]),
        pltpu.make_async_copy(mats_hbm, mats, l_sem.at[2]),
        pltpu.make_async_copy(obj_hbm.at[0], G.at[0, 1, 1], l_sem.at[3]),
        pltpu.make_async_copy(obj_hbm.at[1], G.at[1, 1, 1], l_sem.at[4]),
    ]
    for i in (3, 4, 0, 1, 2):
        local[i].start()

    barrier = pltpu.get_barrier_semaphore()

    def greet(row, col):
        pl.semaphore_signal(
            barrier, inc=1, device_id={"rows": row, "cols": col}, device_id_type=MESH
        )

    greet(rc, c)
    greet(r, cp)

    @pl.when(has_x)
    def _():
        greet(rx, c)

    @pl.when(has_cx)
    def _():
        greet(r, cx)

    @pl.when(has_far)
    def _():
        greet(r, cf)

    always = None

    def both(a, b):
        return a & b

    def when(cond, f):
        if cond is None:
            f()
        else:
            pl.when(cond)(f)

    g_sends = {2: has_x, 3: has_x, 4: has_cx, 5: both(has_x, has_far), 7: has_far}
    g_recvs = {2: has_x, 3: has_x, 4: has_far, 5: both(has_x, has_far), 7: has_far}

    def g_copy(L, k, q):
        src, dst, dev = {
            0: ((1, 1), (2 - rcs, 1), (rc, c)),
            1: ((1, 1), (1, 2 - hp), (r, cp)),
            2: ((1, 1), (2 - rxs, 1), (rx, c)),
            3: ((1, hp), (2 - rxs, hp), (rx, c)),
            4: ((1, hp), (1, fp), (r, cx)),
            5: ((1, fp), (2 - rxs, fp), (rx, c)),
            6: ((1, hp), (2 - rcs, hp), (rc, c)),
            7: ((1, fp), (2 - rcs, fp), (rc, c)),
        }[k]
        part = (pl.ds(q * CHUNK, CHUNK),)
        return pltpu.make_async_remote_copy(
            src_ref=G.at[(L,) + src + part],
            dst_ref=G.at[(L,) + dst + part],
            send_sem=g_send.at[L, k, q],
            recv_sem=g_recv.at[L, k, q],
            device_id={"rows": dev[0], "cols": dev[1]},
            device_id_type=MESH,
        )

    def g_start(L, k, q):
        when(g_sends.get(k, always), lambda: g_copy(L, k, q).start())

    def g_wait(L, k, q):
        when(g_recvs.get(k, always), lambda: g_copy(L, k, q).wait_recv())

    def chunks(planes):
        return [(L, q) for L in planes for q in range(T // CHUNK)]

    def start_all(copy, sends, planes, k):
        def go():
            for L, q in chunks(planes):
                copy(L, k, q).start()

        when(sends.get(k, always), go)

    def g_begin(planes, kinds):
        for k in kinds:
            start_all(g_copy, g_sends, planes, k)

    def g_finish(it, meanwhile=None):
        planes = (2 * it, 2 * it + 1)
        for L, q in chunks(planes):
            g_wait(L, 1, q)
            g_start(L, 4, q)
            g_start(L, 6, q)
            g_start(L, 3, q)
        if meanwhile is not None:
            meanwhile()

        @pl.when(has_far)
        def _():
            for L, q in chunks(planes):
                g_copy(L, 4, q).wait_recv()
                g_copy(L, 7, q).start()
                g_start(L, 5, q)

        every(before, 2, it)
        for L, q in chunks(planes):
            g_wait(L, 0, q)
            g_wait(L, 6, q)

        @pl.when(has_x)
        def _():
            for L, q in chunks(planes):
                g_copy(L, 2, q).wait_recv()
                g_copy(L, 3, q).wait_recv()

        @pl.when(has_far)
        def _():
            for L, q in chunks(planes):
                g_copy(L, 7, q).wait_recv()
                g_wait(L, 5, q)

    f_sends = {1: has_far, 2: has_x, 4: has_x, 5: has_x}
    f_recvs = {1: has_cx, 2: has_x, 4: has_x, 5: has_x}

    def f_copy(L, k, q):
        part = pl.ds(q * CHUNK, CHUNK)
        src, dst, dev = {
            0: (A.at[L, rcs, fp, part], FC.at[L, fp, part], (rc, c)),
            6: (A.at[L, rcs, hp, part], FC.at[L, hp, part], (rc, c)),
            7: (A.at[L, rcs, 1, part], FC.at[L, 1, part], (rc, c)),
            2: (A.at[L, rxs, fp, part], FR.at[L, fp, part], (rx, c)),
            5: (A.at[L, rxs, hp, part], FR.at[L, hp, part], (rx, c)),
            4: (A.at[L, rxs, 1, part], FR.at[L, 1, part], (rx, c)),
            1: (A.at[L, 1, fp, part], FX.at[L, part], (r, cf)),
            3: (A.at[L, 1, hp, part], FY.at[L, part], (r, cp)),
        }[k]
        return pltpu.make_async_remote_copy(
            src_ref=src,
            dst_ref=dst,
            send_sem=f_send.at[L, k, q],
            recv_sem=f_recv.at[L, k, q],
            device_id={"rows": dev[0], "cols": dev[1]},
            device_id_type=MESH,
        )

    def f_start(L, k, q):
        when(f_sends.get(k, always), lambda: f_copy(L, k, q).start())

    def f_wait(L, k, q):
        when(f_recvs.get(k, always), lambda: f_copy(L, k, q).wait_recv())

    def f_begin(planes, kinds=(0, 2, 6, 5, 7, 4)):
        for k in kinds:
            start_all(f_copy, f_sends, planes, k)

    def f_core(planes):
        for L, q in chunks(planes):
            part = pl.ds(q * CHUNK, CHUNK)
            f_wait(L, 0, q)
            f_wait(L, 2, q)
            A[L, 1, fp, part] += FC[L, fp, part] + FR[L, fp, part]
            f_start(L, 1, q)
        for L, q in chunks(planes):
            part = pl.ds(q * CHUNK, CHUNK)
            f_wait(L, 6, q)
            f_wait(L, 5, q)
            A[L, 1, hp, part] += FC[L, hp, part] + FR[L, hp, part]

    def f_across(planes):
        for L, q in chunks(planes):
            part = pl.ds(q * CHUNK, CHUNK)
            f_wait(L, 1, q)
            A[L, 1, hp, part] += FX[L, part]
            f_start(L, 3, q)

    def f_end(L, q):
        part = pl.ds(q * CHUNK, CHUNK)
        for k in (7, 4, 3):
            f_wait(L, k, q)
        return A[L, 1, 1, part] + FC[L, 1, part] + FR[L, 1, part] + FY[L, part]

    local[3].wait()
    local[4].wait()
    greeted = 2 + has_x.astype(jnp.int32) + has_cx.astype(jnp.int32) + has_far.astype(jnp.int32)
    pl.semaphore_wait(barrier, greeted)
    g_begin((0, 1), (1, 2, 0))

    zero_tile = jnp.zeros((T, T), f32)

    @pl.when(jnp.logical_not(has_x))
    def _():
        for L in range(2 * ITERS):
            for col in range(3):
                G[L, rxs, col] = zero_tile
        for L in range(2 * ITERS + 1):
            for col in range(3):
                FR[L, col] = zero_tile

    @pl.when(jnp.logical_not(has_cx))
    def _():
        for L in range(2 * ITERS + 1):
            FX[L] = zero_tile

    @pl.when(jnp.logical_not(has_far))
    def _():
        for L in range(2 * ITERS):
            for row in range(3):
                G[L, row, fp] = zero_tile

    for L in range(2 * ITERS + 1):
        for row in range(3):
            for col in range(3):
                A[L, row, col] = zero_tile

    row_of = lax.broadcasted_iota(jnp.int32, (T, T), 0)
    col_of = lax.broadcasted_iota(jnp.int32, (T, T), 1)

    def add_rows(L, p, i, term):
        mr = row_of >= off_ref[0, p]
        mc = col_of >= off_ref[1, p]
        zero = jnp.zeros((T, T), f32)
        if i == 0:
            top = jnp.where(mr, term[0], zero)
            low = jnp.where(mr, zero, term[0])
            A[L, 0, 0] += jnp.where(mc, top, zero)
            A[L, 0, 2] += jnp.where(mc, zero, top)
            A[L, 2, 0] += jnp.where(mc, low, zero)
            A[L, 2, 2] += jnp.where(mc, zero, low)
            A[L, 0, 1] += jnp.where(mr, term[1], zero)
            A[L, 2, 1] += jnp.where(mr, zero, term[1])
        else:
            A[L, 1, 0] += jnp.where(mc, term[0], zero)
            A[L, 1, 2] += jnp.where(mc, zero, term[0])
            A[L, 1, 1] += term[1]

    local[0].wait()

    def roll_probe(p, carry):
        power = None
        for plane in range(2):
            x = pltpu.roll(probe[plane], off_ref[0, p], 0)
            x = pltpu.roll(x, off_ref[1, p], 1)
            rolled[p, plane] = x
            power = x * x if power is None else power + x * x
        for i in range(2):
            rows = power[i * T:(i + 1) * T]
            add_rows(2 * ITERS, p, i, [rows[:, :T], rows[:, T:]])
        return carry

    lax.fori_loop(0, n_pos, roll_probe, 0)
    light = (2 * ITERS,)
    f_begin(light)

    local[1].wait()
    lane_in = lax.broadcasted_iota(jnp.int32, (W, W), 0)
    lane_out = lax.broadcasted_iota(jnp.int32, (W, W), 1)
    source = jnp.where(lane_out < T, 2 * lane_out, 2 * lane_out - (W - 1))
    perm = jnp.where(lane_in == source, 1.0, 0.0).astype(bf16)

    def permute_amp(p, carry):
        x = amp[p]
        hi = x.astype(bf16)
        mid, low = split(x - hi.astype(f32))
        x = mm(hi, perm) + mm(mid, perm) + mm(low, perm)
        for half in range(2):
            lanes = pl.ds(half * T, T)
            halves[half] = x[:, half * T:(half + 1) * T]
            for par in range(2):
                ampp[p, par, :, lanes] = halves[half, pl.ds(par, T, stride=2), :]
        return carry

    lax.fori_loop(0, n_pos, permute_amp, 0)
    local[2].wait()

    def right(x, m):
        hi, lo = split(x)
        return mm(hi, mats[m]) + mm(lo, mats[m]) + mm(hi, mats[m + 1])

    def left(m, x):
        hi, lo = split(x)
        return mm(mats[m], hi) + mm(mats[m + 1], hi) + mm(mats[m], lo)

    def exit_rows(it, p, i):
        mr = row_of >= off_ref[0, p]
        mc = col_of >= off_ref[1, p]
        ob = []
        for L in (2 * it, 2 * it + 1):
            t = lambda a, b: G[L, a, b]
            if i == 0:
                ob.append([
                    jnp.where(mr, jnp.where(mc, t(0, 0), t(0, 2)), jnp.where(mc, t(2, 0), t(2, 2))),
                    jnp.where(mr, t(0, 1), t(2, 1)),
                ])
            else:
                ob.append([jnp.where(mc, t(1, 0), t(1, 2)), t(1, 1)])
        rows = slice(i * T, (i + 1) * T)
        pr = [rolled[p, 0, rows, :T], rolled[p, 0, rows, T:]]
        pi = [rolled[p, 1, rows, :T], rolled[p, 1, rows, T:]]
        er = [pr[j] * ob[0][j] - pi[j] * ob[1][j] for j in range(2)]
        ei = [pr[j] * ob[1][j] + pi[j] * ob[0][j] for j in range(2)]
        u = jnp.concatenate([er[0] + er[1], ei[0] + ei[1]], 1)
        v = jnp.concatenate([er[0] - er[1], ei[0] - ei[1]], 1)
        return right(u, 0), right(v, 2)

    def back_rows(zr, zi):
        even = right(jnp.concatenate([zr[:, :T], zi[:, :T]], 1), 4)
        odd = right(jnp.concatenate([zr[:, T:], zi[:, T:]], 1), 6)
        return even, odd

    def terms(p, i, even, odd):
        tot, dif = even + odd, even - odd
        br = [tot[:, :T], dif[:, :T]]
        bi = [tot[:, T:], dif[:, T:]]
        rows = slice(i * T, (i + 1) * T)
        pr = [rolled[p, 0, rows, :T], rolled[p, 0, rows, T:]]
        pi = [rolled[p, 1, rows, :T], rolled[p, 1, rows, T:]]
        return (
            [pr[j] * br[j] + pi[j] * bi[j] for j in range(2)],
            [pr[j] * bi[j] - pi[j] * br[j] for j in range(2)],
        )

    def before(it, p):
        even, odd = exit_rows(it, p, 1)
        yield
        held[p, 0] = even
        held[p, 1] = odd
        yield

    def window(it, p):
        even, odd = exit_rows(it, p, 0)
        yield
        low_even, low_odd = held[p, 0], held[p, 1]
        yr = [jnp.concatenate([e[:, :T], o[:, :T]], 1) for e, o in ((even, odd), (low_even, low_odd))]
        yi = [jnp.concatenate([e[:, T:], o[:, T:]], 1) for e, o in ((even, odd), (low_even, low_odd))]
        u = jnp.concatenate([yr[0] + yr[1], yi[0] + yi[1]], 0)
        v = jnp.concatenate([yr[0] - yr[1], yi[0] - yi[1]], 0)
        back = []
        fars = [left(4 + 2 * par, x) for par, x in ((0, u), (1, v))]
        yield
        for par, far in enumerate(fars):
            fr, fi = far[:T], far[T:]
            keep = 1.0 - ampp[p, par] * lax.rsqrt(jnp.maximum(fr * fr + fi * fi, 0.25))
            back.append(left(2 * par, jnp.concatenate([fr * keep, fi * keep], 0)))
        yield
        tot, dif = back[0] + back[1], back[0] - back[1]
        held[p, 0] = dif[:T]
        held[p, 1] = dif[T:]
        even, odd = back_rows(tot[:T], tot[T:])
        yield
        for L, term in zip((2 * it, 2 * it + 1), terms(p, 0, even, odd)):
            add_rows(L, p, 0, term)
        yield

    def after(it, p):
        even, odd = back_rows(held[p, 0], held[p, 1])
        yield
        for L, term in zip((2 * it, 2 * it + 1), terms(p, 1, even, odd)):
            add_rows(L, p, 1, term)
        yield

    def every(part, stages, it):
        def step(t, carry):
            running = [part(it, GROUP * t + i) for i in range(GROUP)]
            for _ in range(stages):
                for one in running:
                    next(one)
            return carry

        lax.fori_loop(0, n_pos // GROUP, step, 0)

    g_finish(0, lambda: f_core(light))
    f_across(light)
    for it in range(ITERS):
        planes = (2 * it, 2 * it + 1)
        every(window, 5, it)
        f_begin(planes)
        every(after, 2, it)
        if it == 0:
            for _, q in chunks(light):
                ill[pl.ds(q * CHUNK, CHUNK)] = f_end(2 * ITERS, q) + 1.0
        f_core(planes)
        f_across(planes)
        for L, q in chunks(planes):
            part = pl.ds(q * CHUNK, CHUNK)
            new = G[L, 1, 1, part] - f_end(L, q) / ill[part]
            if it < ITERS - 1:
                G[L + 2, 1, 1, part] = new
                g_start(L + 2, 1, q)
            else:
                out_ref[L - 2 * it, part] = new
        if it < ITERS - 1:
            planes = (2 * it + 2, 2 * it + 3)
            g_begin(planes, (2, 0))
            g_finish(it + 1)

    for copy, sends, planes in ((g_copy, g_sends, 2 * ITERS), (f_copy, f_sends, 2 * ITERS + 1)):
        for k in range(8):

            def drain():
                for L, q in chunks(range(planes)):
                    copy(L, k, q).wait_send()

            when(sends.get(k, always), drain)


def local(n_rows, n_cols, object_field, probe, amplitudes, offsets):
    n_pos = amplitudes.shape[2]
    n = 2 * ITERS

    def fix(x):
        return pltpu.with_memory_space_constraint(x, pltpu.HBM)

    hbm = pl.BlockSpec(memory_space=pltpu.HBM)
    vmem = pl.BlockSpec(memory_space=pltpu.VMEM)
    return pl.pallas_call(
        functools.partial(kernel, n_rows, n_cols, n_pos),
        out_shape=jax.ShapeDtypeStruct(object_field.shape, f32),
        in_specs=[hbm, pl.BlockSpec(memory_space=pltpu.SMEM), hbm, hbm, hbm],
        out_specs=vmem,
        scratch_shapes=[
            pltpu.VMEM((n, 3, 3, T, T), f32),
            pltpu.VMEM((n + 1, 3, 3, T, T), f32),
            pltpu.VMEM((n + 1, 3, T, T), f32),
            pltpu.VMEM((n + 1, 3, T, T), f32),
            pltpu.VMEM((n + 1, T, T), f32),
            pltpu.VMEM((n + 1, T, T), f32),
            pltpu.VMEM((T, T), f32),
            pltpu.VMEM((2, W, W), f32),
            pltpu.VMEM((n_pos, W, W), f32),
            pltpu.VMEM((8, W, W), bf16),
            pltpu.VMEM((n_pos, 2, W, W), f32),
            pltpu.VMEM((n_pos, 2, T, W), f32),
            pltpu.VMEM((2, W, T), f32),
            pltpu.VMEM((n_pos, 2, T, W), f32),
            pltpu.SemaphoreType.DMA((n, 8, T // CHUNK)),
            pltpu.SemaphoreType.DMA((n, 8, T // CHUNK)),
            pltpu.SemaphoreType.DMA((n + 1, 8, T // CHUNK)),
            pltpu.SemaphoreType.DMA((n + 1, 8, T // CHUNK)),
            pltpu.SemaphoreType.DMA((5,)),
        ],
        compiler_params=pltpu.CompilerParams(
            collective_id=0, has_side_effects=True, vmem_limit_bytes=VMEM_MIB * 1024 * 1024
        ),
    )(
        fix(object_field),
        fix(offsets[0, 0].T),
        fix(probe),
        fix(amplitudes[0, 0]),
        fix(jnp.asarray(dft_parts())),
    )


def solution(mesh):
    placed = (
        P(None, "rows", "cols"),
        P(),
        P("rows", "cols", None, None, None),
        P("rows", "cols", None, None),
    )
    body = functools.partial(local, mesh.shape["rows"], mesh.shape["cols"])
    return jax.shard_map(
        body, mesh=mesh, in_specs=placed, out_specs=P(None, "rows", "cols"), check_vma=False
    )
```

```python
import functools
import math

import jax
import jax.numpy as jnp
import numpy as np
from jax import lax
from jax.experimental import pallas as pl
from jax.experimental.pallas import tpu as pltpu
from jax.sharding import PartitionSpec as P

ITERS = 2
T = 128
W = 256
CHUNK = 64
GROUP = 4
VMEM_MIB = 28
MESH = pl.DeviceIdType.MESH
f32 = jnp.float32
bf16 = jnp.bfloat16


def dft_parts():
    m = np.arange(T)
    mats = []
    for odd in (0, 1):
        turns = (m[:, None] * (2 * m[None, :] + odd)) % W
        angle = 2.0 * np.pi / W * turns
        c, s = np.cos(angle) / 16.0, np.sin(angle) / 16.0
        mats.append(np.block([[c, -s], [s, c]]))
    mats = [mats[0], mats[1], mats[0].T, mats[1].T]
    out = []
    for a in mats:
        a = a.astype(np.float32)
        hi = a.astype(jnp.bfloat16)
        lo = (a - hi.astype(np.float32)).astype(jnp.bfloat16)
        out += [hi, lo]
    return np.stack(out)


def split(x):
    hi = x.astype(bf16)
    return hi, (x - hi.astype(f32)).astype(bf16)


def mm(a, b):
    return jnp.dot(a, b, preferred_element_type=f32)


def kernel(
    n_rows, n_cols, n_pos,
    obj_hbm, off_ref, probe_hbm, amp_hbm, mats_hbm,
    out_ref,
    G, A, FC, FR, FX, FY, ill, probe, amp, mats, rolled, ampp, halves, held,
    g_send, g_recv, f_send, f_recv, l_sem,
):
    r = lax.axis_index("rows")
    c = lax.axis_index("cols")
    ro, h = lax.rem(r, 2), lax.rem(c, 2)
    rc, rx = r + 1 - 2 * ro, r - 1 + 2 * ro
    cp = c + 1 - 2 * h
    cx, cf = c + 2 - 4 * h, c - 2 + 4 * h
    has_x = (rx >= 0) & (rx < n_rows)
    has_cx = (cx >= 0) & (cx < n_cols)
    has_far = (cf >= 0) & (cf < n_cols)
    rcs = rc - r + 1
    rxs = 2 - rcs
    hp = cp - c + 1
    fp = 2 - hp

    local = [
        pltpu.make_async_copy(probe_hbm, probe, l_sem.at[0]),
        pltpu.make_async_copy(amp_hbm, amp, l_sem.at[1]),
        pltpu.make_async_copy(mats_hbm, mats, l_sem.at[2]),
        pltpu.make_async_copy(obj_hbm.at[0], G.at[0, 1, 1], l_sem.at[3]),
        pltpu.make_async_copy(obj_hbm.at[1], G.at[1, 1, 1], l_sem.at[4]),
    ]
    for i in (3, 4, 0, 1, 2):
        local[i].start()

    barrier = pltpu.get_barrier_semaphore()

    def greet(row, col):
        pl.semaphore_signal(
            barrier, inc=1, device_id={"rows": row, "cols": col}, device_id_type=MESH
        )

    greet(rc, c)
    greet(r, cp)

    @pl.when(has_x)
    def _():
        greet(rx, c)

    @pl.when(has_cx)
    def _():
        greet(r, cx)

    @pl.when(has_far)
    def _():
        greet(r, cf)

    always = None

    def both(a, b):
        return a & b

    def when(cond, f):
        if cond is None:
            f()
        else:
            pl.when(cond)(f)

    def tile(ph, L, q):
        if L is None:
            n = 2 if ph < ITERS else 1
            return pl.ds(2 * ph, n), ()
        return L, (pl.ds(q * CHUNK, CHUNK),)

    def chunks(ph):
        n = 2 if ph < ITERS else 1
        return [(2 * ph + i, q) for i in range(n) for q in range(T // CHUNK)]

    def remote(src, dst, send, recv, ph, L, q, k, dev):
        return pltpu.make_async_remote_copy(
            src_ref=src,
            dst_ref=dst,
            send_sem=send.at[ph, k],
            recv_sem=recv.at[2 * ph, k, 0] if L is None else recv.at[L, k, q],
            device_id={"rows": dev[0], "cols": dev[1]},
            device_id_type=MESH,
        )

    g_sends = {2: has_x, 3: has_x, 4: has_cx, 5: both(has_x, has_far), 7: has_far}

    def g_copy(ph, k, L=None, q=None):
        src, dst, dev = {
            0: ((1, 1), (2 - rcs, 1), (rc, c)),
            1: ((1, 1), (1, 2 - hp), (r, cp)),
            2: ((1, 1), (2 - rxs, 1), (rx, c)),
            3: ((1, hp), (2 - rxs, hp), (rx, c)),
            4: ((1, hp), (1, fp), (r, cx)),
            5: ((1, fp), (2 - rxs, fp), (rx, c)),
            6: ((1, hp), (2 - rcs, hp), (rc, c)),
            7: ((1, fp), (2 - rcs, fp), (rc, c)),
        }[k]
        lead, part = tile(ph, L, q)
        return remote(
            G.at[(lead,) + src + part], G.at[(lead,) + dst + part], g_send, g_recv, ph, L, q, k, dev
        )

    def g_begin(ph):
        g_copy(ph, 0).start()
        pl.when(has_x)(lambda: g_copy(ph, 2).start())

    def g_finish(ph, meanwhile=None):
        for L, q in chunks(ph):
            g_copy(ph, 1, L, q).wait_recv()
            pl.when(has_cx)(lambda: g_copy(ph, 4, L, q).start())
        g_copy(ph, 6).start()
        pl.when(has_x)(lambda: g_copy(ph, 3).start())
        if meanwhile is not None:
            meanwhile()

        @pl.when(has_far)
        def _():
            for L, q in chunks(ph):
                g_copy(ph, 4, L, q).wait_recv()
                pl.when(has_x)(lambda: g_copy(ph, 5, L, q).start())
                g_copy(ph, 7, L, q).start()

        every(before, 2, ph)
        g_copy(ph, 0).wait_recv()
        g_copy(ph, 6).wait_recv()

        @pl.when(has_x)
        def _():
            g_copy(ph, 2).wait_recv()
            g_copy(ph, 3).wait_recv()

        @pl.when(has_far)
        def _():
            for L, q in chunks(ph):
                g_copy(ph, 7, L, q).wait_recv()
                pl.when(has_x)(lambda: g_copy(ph, 5, L, q).wait_recv())

    f_sends = {1: has_far, 2: has_x, 4: has_x, 5: has_x}

    def f_copy(ph, k, L=None, q=None):
        lead, part = tile(ph, L, q)
        src, dst, dev = {
            0: (A.at[(lead, rcs, fp) + part], FC.at[(lead, fp) + part], (rc, c)),
            6: (A.at[(lead, rcs, hp) + part], FC.at[(lead, hp) + part], (rc, c)),
            7: (A.at[(lead, rcs, 1) + part], FC.at[(lead, 1) + part], (rc, c)),
            2: (A.at[(lead, rxs, fp) + part], FR.at[(lead, fp) + part], (rx, c)),
            5: (A.at[(lead, rxs, hp) + part], FR.at[(lead, hp) + part], (rx, c)),
            4: (A.at[(lead, rxs, 1) + part], FR.at[(lead, 1) + part], (rx, c)),
            1: (A.at[(lead, 1, fp) + part], FX.at[(lead,) + part], (r, cf)),
            3: (A.at[(lead, 1, hp) + part], FY.at[(lead,) + part], (r, cp)),
        }[k]
        return remote(src, dst, f_send, f_recv, ph, L, q, k, dev)

    def f_begin(ph):
        @pl.when(has_x)
        def _():
            for L, q in chunks(ph):
                f_copy(ph, 2, L, q).start()
            f_copy(ph, 5).start()
            f_copy(ph, 4).start()

        for L, q in chunks(ph):
            f_copy(ph, 0, L, q).start()
        f_copy(ph, 6).start()
        f_copy(ph, 7).start()

    def f_core(ph):
        for L, q in chunks(ph):
            part = pl.ds(q * CHUNK, CHUNK)
            f_copy(ph, 0, L, q).wait_recv()
            pl.when(has_x)(lambda: f_copy(ph, 2, L, q).wait_recv())
            A[L, 1, fp, part] += FC[L, fp, part] + FR[L, fp, part]
            pl.when(has_far)(lambda: f_copy(ph, 1, L, q).start())
        f_copy(ph, 6).wait_recv()
        pl.when(has_x)(lambda: f_copy(ph, 5).wait_recv())
        for L, q in chunks(ph):
            part = pl.ds(q * CHUNK, CHUNK)
            A[L, 1, hp, part] += FC[L, hp, part] + FR[L, hp, part]

    def f_across(ph):
        for L, q in chunks(ph):
            part = pl.ds(q * CHUNK, CHUNK)
            pl.when(has_cx)(lambda: f_copy(ph, 1, L, q).wait_recv())
            A[L, 1, hp, part] += FX[L, part]
            f_copy(ph, 3, L, q).start()
        f_copy(ph, 7).wait_recv()
        pl.when(has_x)(lambda: f_copy(ph, 4).wait_recv())
        for L, q in chunks(ph):
            part = pl.ds(q * CHUNK, CHUNK)
            A[L, 1, 1, part] += FC[L, 1, part] + FR[L, 1, part]

    def f_end(ph, L, q):
        part = pl.ds(q * CHUNK, CHUNK)
        f_copy(ph, 3, L, q).wait_recv()
        return A[L, 1, 1, part] + FY[L, part]

    def drain(copy, sends, ph):
        for k in range(8):
            when(sends.get(k, always), lambda: copy(ph, k).wait_send())

    local[3].wait()
    local[4].wait()
    greeted = 2 + has_x.astype(jnp.int32) + has_cx.astype(jnp.int32) + has_far.astype(jnp.int32)
    pl.semaphore_wait(barrier, greeted)
    for L, q in chunks(0):
        g_copy(0, 1, L, q).start()
    g_begin(0)

    zero_tile = jnp.zeros((T, T), f32)

    @pl.when(jnp.logical_not(has_x))
    def _():
        for L in range(2 * ITERS):
            for col in range(3):
                G[L, rxs, col] = zero_tile
        for L in range(2 * ITERS + 1):
            for col in range(3):
                FR[L, col] = zero_tile

    @pl.when(jnp.logical_not(has_cx))
    def _():
        for L in range(2 * ITERS + 1):
            FX[L] = zero_tile

    @pl.when(jnp.logical_not(has_far))
    def _():
        for L in range(2 * ITERS):
            for row in range(3):
                G[L, row, fp] = zero_tile

    for L in range(2 * ITERS + 1):
        for row in range(3):
            for col in range(3):
                A[L, row, col] = zero_tile

    row_of = lax.broadcasted_iota(jnp.int32, (T, T), 0)
    col_of = lax.broadcasted_iota(jnp.int32, (T, T), 1)

    def add_rows(L, p, i, term):
        mr = row_of >= off_ref[0, p]
        mc = col_of >= off_ref[1, p]
        zero = jnp.zeros((T, T), f32)
        if i == 0:
            top = jnp.where(mr, term[0], zero)
            low = jnp.where(mr, zero, term[0])
            A[L, 0, 0] += jnp.where(mc, top, zero)
            A[L, 0, 2] += jnp.where(mc, zero, top)
            A[L, 2, 0] += jnp.where(mc, low, zero)
            A[L, 2, 2] += jnp.where(mc, zero, low)
            A[L, 0, 1] += jnp.where(mr, term[1], zero)
            A[L, 2, 1] += jnp.where(mr, zero, term[1])
        else:
            A[L, 1, 0] += jnp.where(mc, term[0], zero)
            A[L, 1, 2] += jnp.where(mc, zero, term[0])
            A[L, 1, 1] += term[1]

    local[0].wait()

    def roll_probe(p, carry):
        power = None
        for plane in range(2):
            x = pltpu.roll(probe[plane], off_ref[0, p], 0)
            x = pltpu.roll(x, off_ref[1, p], 1)
            rolled[p, plane] = x
            power = x * x if power is None else power + x * x
        for i in range(2):
            rows = power[i * T:(i + 1) * T]
            add_rows(2 * ITERS, p, i, [rows[:, :T], rows[:, T:]])
        return carry

    lax.fori_loop(0, n_pos, roll_probe, 0)
    light = ITERS
    f_begin(light)

    local[1].wait()
    lane_in = lax.broadcasted_iota(jnp.int32, (W, W), 0)
    lane_out = lax.broadcasted_iota(jnp.int32, (W, W), 1)
    source = jnp.where(lane_out < T, 2 * lane_out, 2 * lane_out - (W - 1))
    perm = jnp.where(lane_in == source, 1.0, 0.0).astype(bf16)

    def permute_amp(p, carry):
        x = amp[p]
        hi = x.astype(bf16)
        mid, low = split(x - hi.astype(f32))
        x = mm(hi, perm) + mm(mid, perm) + mm(low, perm)
        for half in range(2):
            lanes = pl.ds(half * T, T)
            halves[half] = x[:, half * T:(half + 1) * T]
            for par in range(2):
                ampp[p, par, :, lanes] = halves[half, pl.ds(par, T, stride=2), :]
        return carry

    lax.fori_loop(0, n_pos, permute_amp, 0)
    local[2].wait()

    def right(x, m):
        hi, lo = split(x)
        return mm(hi, mats[m]) + mm(lo, mats[m]) + mm(hi, mats[m + 1])

    def left(m, x):
        hi, lo = split(x)
        return mm(mats[m], hi) + mm(mats[m + 1], hi) + mm(mats[m], lo)

    def exit_rows(it, p, i):
        mr = row_of >= off_ref[0, p]
        mc = col_of >= off_ref[1, p]
        ob = []
        for L in (2 * it, 2 * it + 1):
            t = lambda a, b: G[L, a, b]
            if i == 0:
                ob.append([
                    jnp.where(mr, jnp.where(mc, t(0, 0), t(0, 2)), jnp.where(mc, t(2, 0), t(2, 2))),
                    jnp.where(mr, t(0, 1), t(2, 1)),
                ])
            else:
                ob.append([jnp.where(mc, t(1, 0), t(1, 2)), t(1, 1)])
        rows = slice(i * T, (i + 1) * T)
        pr = [rolled[p, 0, rows, :T], rolled[p, 0, rows, T:]]
        pi = [rolled[p, 1, rows, :T], rolled[p, 1, rows, T:]]
        er = [pr[j] * ob[0][j] - pi[j] * ob[1][j] for j in range(2)]
        ei = [pr[j] * ob[1][j] + pi[j] * ob[0][j] for j in range(2)]
        u = jnp.concatenate([er[0] + er[1], ei[0] + ei[1]], 1)
        v = jnp.concatenate([er[0] - er[1], ei[0] - ei[1]], 1)
        return right(u, 0), right(v, 2)

    def back_rows(zr, zi):
        even = right(jnp.concatenate([zr[:, :T], zi[:, :T]], 1), 4)
        odd = right(jnp.concatenate([zr[:, T:], zi[:, T:]], 1), 6)
        return even, odd

    def terms(p, i, even, odd):
        tot, dif = even + odd, even - odd
        br = [tot[:, :T], dif[:, :T]]
        bi = [tot[:, T:], dif[:, T:]]
        rows = slice(i * T, (i + 1) * T)
        pr = [rolled[p, 0, rows, :T], rolled[p, 0, rows, T:]]
        pi = [rolled[p, 1, rows, :T], rolled[p, 1, rows, T:]]
        return (
            [pr[j] * br[j] + pi[j] * bi[j] for j in range(2)],
            [pr[j] * bi[j] - pi[j] * br[j] for j in range(2)],
        )

    def before(it, p):
        even, odd = exit_rows(it, p, 1)
        yield
        held[p, 0] = even
        held[p, 1] = odd
        yield

    def window(it, p):
        even, odd = exit_rows(it, p, 0)
        yield
        low_even, low_odd = held[p, 0], held[p, 1]
        yr = [jnp.concatenate([e[:, :T], o[:, :T]], 1) for e, o in ((even, odd), (low_even, low_odd))]
        yi = [jnp.concatenate([e[:, T:], o[:, T:]], 1) for e, o in ((even, odd), (low_even, low_odd))]
        u = jnp.concatenate([yr[0] + yr[1], yi[0] + yi[1]], 0)
        v = jnp.concatenate([yr[0] - yr[1], yi[0] - yi[1]], 0)
        back = []
        fars = [left(4 + 2 * par, x) for par, x in ((0, u), (1, v))]
        yield
        for par, far in enumerate(fars):
            fr, fi = far[:T], far[T:]
            keep = 1.0 - ampp[p, par] * lax.rsqrt(jnp.maximum(fr * fr + fi * fi, 0.25))
            back.append(left(2 * par, jnp.concatenate([fr * keep, fi * keep], 0)))
        yield
        tot, dif = back[0] + back[1], back[0] - back[1]
        held[p, 0] = dif[:T]
        held[p, 1] = dif[T:]
        even, odd = back_rows(tot[:T], tot[T:])
        yield
        for L, term in zip((2 * it, 2 * it + 1), terms(p, 0, even, odd)):
            add_rows(L, p, 0, term)
        yield

    def after(it, p):
        even, odd = back_rows(held[p, 0], held[p, 1])
        yield
        for L, term in zip((2 * it, 2 * it + 1), terms(p, 1, even, odd)):
            add_rows(L, p, 1, term)
        yield

    def every(part, stages, it):
        def step(t, carry):
            running = [part(it, GROUP * t + i) for i in range(GROUP)]
            for _ in range(stages):
                for one in running:
                    next(one)
            return carry

        lax.fori_loop(0, n_pos // GROUP, step, 0)

    g_finish(0, lambda: f_core(light))
    f_across(light)
    for it in range(ITERS):
        every(window, 5, it)
        f_begin(it)
        every(after, 2, it)
        if it == 0:
            for L, q in chunks(light):
                ill[pl.ds(q * CHUNK, CHUNK)] = f_end(light, L, q) + 1.0
        f_core(it)
        if it == ITERS - 1:
            drain(f_copy, f_sends, light)
            for done in range(ITERS):
                drain(g_copy, g_sends, done)
            for done in range(ITERS - 1):
                drain(f_copy, f_sends, done)
        f_across(it)
        for L, q in chunks(it):
            part = pl.ds(q * CHUNK, CHUNK)
            new = G[L, 1, 1, part] - f_end(it, L, q) / ill[part]
            if it < ITERS - 1:
                G[L + 2, 1, 1, part] = new
                g_copy(it + 1, 1, L + 2, q).start()
            else:
                out_ref[L - 2 * it, part] = new
        if it < ITERS - 1:
            g_begin(it + 1)
            g_finish(it + 1)
    drain(f_copy, f_sends, ITERS - 1)


def local(n_rows, n_cols, object_field, probe, amplitudes, offsets):
    n_pos = amplitudes.shape[2]
    n = 2 * ITERS

    def fix(x):
        return pltpu.with_memory_space_constraint(x, pltpu.HBM)

    hbm = pl.BlockSpec(memory_space=pltpu.HBM)
    vmem = pl.BlockSpec(memory_space=pltpu.VMEM)
    return pl.pallas_call(
        functools.partial(kernel, n_rows, n_cols, n_pos),
        out_shape=jax.ShapeDtypeStruct(object_field.shape, f32),
        in_specs=[hbm, pl.BlockSpec(memory_space=pltpu.SMEM), hbm, hbm, hbm],
        out_specs=vmem,
        scratch_shapes=[
            pltpu.VMEM((n, 3, 3, T, T), f32),
            pltpu.VMEM((n + 1, 3, 3, T, T), f32),
            pltpu.VMEM((n + 1, 3, T, T), f32),
            pltpu.VMEM((n + 1, 3, T, T), f32),
            pltpu.VMEM((n + 1, T, T), f32),
            pltpu.VMEM((n + 1, T, T), f32),
            pltpu.VMEM((T, T), f32),
            pltpu.VMEM((2, W, W), f32),
            pltpu.VMEM((n_pos, W, W), f32),
            pltpu.VMEM((8, W, W), bf16),
            pltpu.VMEM((n_pos, 2, W, W), f32),
            pltpu.VMEM((n_pos, 2, T, W), f32),
            pltpu.VMEM((2, W, T), f32),
            pltpu.VMEM((n_pos, 2, T, W), f32),
            pltpu.SemaphoreType.DMA((ITERS, 8)),
            pltpu.SemaphoreType.DMA((n, 8, T // CHUNK)),
            pltpu.SemaphoreType.DMA((ITERS + 1, 8)),
            pltpu.SemaphoreType.DMA((n + 1, 8, T // CHUNK)),
            pltpu.SemaphoreType.DMA((5,)),
        ],
        compiler_params=pltpu.CompilerParams(
            collective_id=0, has_side_effects=True, vmem_limit_bytes=VMEM_MIB * 1024 * 1024
        ),
    )(
        fix(object_field),
        fix(offsets[0, 0].T),
        fix(probe),
        fix(amplitudes[0, 0]),
        fix(jnp.asarray(dft_parts())),
    )


def solution(mesh):
    placed = (
        P(None, "rows", "cols"),
        P(),
        P("rows", "cols", None, None, None),
        P("rows", "cols", None, None),
    )
    body = functools.partial(local, mesh.shape["rows"], mesh.shape["cols"])
    return jax.shard_map(
        body, mesh=mesh, in_specs=placed, out_specs=P(None, "rows", "cols"), check_vma=False
    )
```

```python
import functools
import math

import jax
import jax.numpy as jnp
import numpy as np
from jax import lax
from jax.experimental import pallas as pl
from jax.experimental.pallas import tpu as pltpu
from jax.sharding import PartitionSpec as P

ITERS = 2
T = 128
W = 256
CHUNK = 64
GROUP = 4
VMEM_MIB = 28
MESH = pl.DeviceIdType.MESH
f32 = jnp.float32
bf16 = jnp.bfloat16


def dft_parts():
    m = np.arange(T)
    mats = []
    for odd in (0, 1):
        turns = (m[:, None] * (2 * m[None, :] + odd)) % W
        angle = 2.0 * np.pi / W * turns
        c, s = np.cos(angle) / 16.0, np.sin(angle) / 16.0
        mats.append(np.block([[c, -s], [s, c]]))
    mats = [mats[0], mats[1], mats[0].T, mats[1].T]
    out = []
    for a in mats:
        a = a.astype(np.float32)
        hi = a.astype(jnp.bfloat16)
        lo = (a - hi.astype(np.float32)).astype(jnp.bfloat16)
        out += [hi, lo]
    return np.stack(out)


def split(x):
    hi = x.astype(bf16)
    return hi, (x - hi.astype(f32)).astype(bf16)


def mm(a, b):
    return jnp.dot(a, b, preferred_element_type=f32)


def kernel(
    n_rows, n_cols, n_pos,
    obj_hbm, off_ref, probe_hbm, amp_hbm, mats_hbm,
    out_ref,
    G, A, FC, FR, FX, FY, ill, probe, amp, mats, rolled, ampp, halves, held,
    g_send, g_recv, f_send, f_recv, l_sem,
):
    r = lax.axis_index("rows")
    c = lax.axis_index("cols")
    ro, h = lax.rem(r, 2), lax.rem(c, 2)
    rc, rx = r + 1 - 2 * ro, r - 1 + 2 * ro
    cp = c + 1 - 2 * h
    cx, cf = c + 2 - 4 * h, c - 2 + 4 * h
    has_x = (rx >= 0) & (rx < n_rows)
    has_cx = (cx >= 0) & (cx < n_cols)
    has_far = (cf >= 0) & (cf < n_cols)
    rcs = rc - r + 1
    rxs = 2 - rcs
    hp = cp - c + 1
    fp = 2 - hp

    barrier = pltpu.get_barrier_semaphore()

    def greet(row, col):
        pl.semaphore_signal(
            barrier, inc=1, device_id={"rows": row, "cols": col}, device_id_type=MESH
        )

    @pl.when(has_cx)
    def _():
        greet(r, cx)

    @pl.when(has_far)
    def _():
        greet(r, cf)

    greet(r, cp)

    @pl.when(has_x)
    def _():
        greet(rx, c)
        greet(rx, cp)

    greet(rc, c)

    local = [
        pltpu.make_async_copy(probe_hbm, probe, l_sem.at[0]),
        pltpu.make_async_copy(amp_hbm, amp, l_sem.at[1]),
        pltpu.make_async_copy(mats_hbm, mats, l_sem.at[2]),
        pltpu.make_async_copy(obj_hbm.at[0], G.at[0, 1, 1], l_sem.at[3]),
        pltpu.make_async_copy(obj_hbm.at[1], G.at[1, 1, 1], l_sem.at[4]),
    ]
    for i in (3, 4, 0, 1, 2):
        local[i].start()

    always = None

    def both(a, b):
        return a & b

    def when(cond, f):
        if cond is None:
            f()
        else:
            pl.when(cond)(f)

    def tile(ph, L, q):
        if L is None:
            n = 2 if ph < ITERS else 1
            return pl.ds(2 * ph, n), ()
        return L, (pl.ds(q * CHUNK, CHUNK),)

    def chunks(ph):
        n = 2 if ph < ITERS else 1
        return [(2 * ph + i, q) for i in range(n) for q in range(T // CHUNK)]

    def remote(src, dst, send, recv, ph, L, q, k, dev):
        return pltpu.make_async_remote_copy(
            src_ref=src,
            dst_ref=dst,
            send_sem=send.at[ph, k],
            recv_sem=recv.at[2 * ph, k, 0] if L is None else recv.at[L, k, q],
            device_id={"rows": dev[0], "cols": dev[1]},
            device_id_type=MESH,
        )

    g_sends = {2: has_x, 3: has_x, 4: has_cx, 5: both(has_x, has_far), 7: has_far}

    def g_copy(ph, k, L=None, q=None):
        src, dst, dev = {
            0: ((1, 1), (2 - rcs, 1), (rc, c)),
            1: ((1, 1), (1, 2 - hp), (r, cp)),
            2: ((1, 1), (2 - rxs, 1), (rx, c)),
            3: ((1, 1), (2 - rxs, 2 - hp), (rx, cp)),
            4: ((1, hp), (1, fp), (r, cx)),
            5: ((1, fp), (2 - rxs, fp), (rx, c)),
            6: ((1, hp), (2 - rcs, hp), (rc, c)),
            7: ((1, fp), (2 - rcs, fp), (rc, c)),
        }[k]
        lead, part = tile(ph, L, q)
        return remote(
            G.at[(lead,) + src + part], G.at[(lead,) + dst + part], g_send, g_recv, ph, L, q, k, dev
        )

    def g_begin(ph):
        g_copy(ph, 0).start()

        @pl.when(has_x)
        def _():
            g_copy(ph, 3).start()
            g_copy(ph, 2).start()


    def g_finish(ph, meanwhile=None):
        for L, q in chunks(ph):
            g_copy(ph, 1, L, q).wait_recv()
            pl.when(has_cx)(lambda: g_copy(ph, 4, L, q).start())
        g_copy(ph, 6).start()
        if meanwhile is not None:
            meanwhile()

        @pl.when(has_far)
        def _():
            for L, q in chunks(ph):
                g_copy(ph, 4, L, q).wait_recv()
                pl.when(has_x)(lambda: g_copy(ph, 5, L, q).start())
                g_copy(ph, 7, L, q).start()

        every(before, 2, ph)
        g_copy(ph, 0).wait_recv()
        g_copy(ph, 6).wait_recv()

        @pl.when(has_x)
        def _():
            g_copy(ph, 2).wait_recv()
            g_copy(ph, 3).wait_recv()

        @pl.when(has_far)
        def _():
            for L, q in chunks(ph):
                g_copy(ph, 7, L, q).wait_recv()
                pl.when(has_x)(lambda: g_copy(ph, 5, L, q).wait_recv())

    f_sends = {1: has_far, 2: has_x, 4: has_x, 5: has_x}

    def f_copy(ph, k, L=None, q=None):
        lead, part = tile(ph, L, q)
        src, dst, dev = {
            0: (A.at[(lead, rcs, fp) + part], FC.at[(lead, fp) + part], (rc, c)),
            6: (A.at[(lead, rcs, hp) + part], FC.at[(lead, hp) + part], (rc, c)),
            7: (A.at[(lead, rcs, 1) + part], FC.at[(lead, 1) + part], (rc, c)),
            2: (A.at[(lead, rxs, fp) + part], FR.at[(lead, fp) + part], (rx, c)),
            5: (A.at[(lead, rxs, hp) + part], FR.at[(lead, 2 - hp) + part], (rx, cp)),
            4: (A.at[(lead, rxs, 1) + part], FR.at[(lead, 1) + part], (rx, c)),
            1: (A.at[(lead, 1, fp) + part], FX.at[(lead,) + part], (r, cf)),
            3: (A.at[(lead, 1, hp) + part], FY.at[(lead,) + part], (r, cp)),
        }[k]
        return remote(src, dst, f_send, f_recv, ph, L, q, k, dev)

    def f_begin(ph):
        @pl.when(has_x)
        def _():
            for L, q in chunks(ph):
                f_copy(ph, 2, L, q).start()
            f_copy(ph, 5).start()

        for L, q in chunks(ph):
            f_copy(ph, 0, L, q).start()
        f_copy(ph, 6).start()
        f_copy(ph, 7).start()

    def f_core(ph):
        for L, q in chunks(ph):
            part = pl.ds(q * CHUNK, CHUNK)
            f_copy(ph, 0, L, q).wait_recv()
            pl.when(has_x)(lambda: f_copy(ph, 2, L, q).wait_recv())
            A[L, 1, fp, part] += FC[L, fp, part] + FR[L, fp, part]
            pl.when(has_far)(lambda: f_copy(ph, 1, L, q).start())
        pl.when(has_x)(lambda: f_copy(ph, 4).start())
        f_copy(ph, 6).wait_recv()
        for L, q in chunks(ph):
            part = pl.ds(q * CHUNK, CHUNK)
            A[L, 1, hp, part] += FC[L, hp, part]

    def f_across(ph):
        for L, q in chunks(ph):
            part = pl.ds(q * CHUNK, CHUNK)
            pl.when(has_cx)(lambda: f_copy(ph, 1, L, q).wait_recv())
            A[L, 1, hp, part] += FX[L, part]
            f_copy(ph, 3, L, q).start()
        f_copy(ph, 7).wait_recv()

        @pl.when(has_x)
        def _():
            f_copy(ph, 4).wait_recv()
            f_copy(ph, 5).wait_recv()

        for L, q in chunks(ph):
            part = pl.ds(q * CHUNK, CHUNK)
            A[L, 1, 1, part] += FC[L, 1, part] + FR[L, 1, part] + FR[L, hp, part]

    def f_end(ph, L, q):
        part = pl.ds(q * CHUNK, CHUNK)
        f_copy(ph, 3, L, q).wait_recv()
        return A[L, 1, 1, part] + FY[L, part]

    def drain(copy, sends, ph):
        for k in range(8):
            when(sends.get(k, always), lambda: copy(ph, k).wait_send())

    local[3].wait()
    local[4].wait()
    greeted = 2 + 2 * has_x.astype(jnp.int32) + has_cx.astype(jnp.int32) + has_far.astype(jnp.int32)
    pl.semaphore_wait(barrier, greeted)
    for L, q in chunks(0):
        g_copy(0, 1, L, q).start()
    g_begin(0)

    zero_tile = jnp.zeros((T, T), f32)

    @pl.when(jnp.logical_not(has_x))
    def _():
        for L in range(2 * ITERS):
            for col in range(3):
                G[L, rxs, col] = zero_tile
        for L in range(2 * ITERS + 1):
            for col in range(3):
                FR[L, col] = zero_tile

    @pl.when(jnp.logical_not(has_cx))
    def _():
        for L in range(2 * ITERS + 1):
            FX[L] = zero_tile

    @pl.when(jnp.logical_not(has_far))
    def _():
        for L in range(2 * ITERS):
            for row in range(3):
                G[L, row, fp] = zero_tile

    for L in range(2 * ITERS + 1):
        for row in range(3):
            for col in range(3):
                A[L, row, col] = zero_tile

    row_of = lax.broadcasted_iota(jnp.int32, (T, T), 0)
    col_of = lax.broadcasted_iota(jnp.int32, (T, T), 1)

    def add_rows(L, p, i, term):
        mr = row_of >= off_ref[0, p]
        mc = col_of >= off_ref[1, p]
        zero = jnp.zeros((T, T), f32)
        if i == 0:
            top = jnp.where(mr, term[0], zero)
            low = jnp.where(mr, zero, term[0])
            A[L, 0, 0] += jnp.where(mc, top, zero)
            A[L, 0, 2] += jnp.where(mc, zero, top)
            A[L, 2, 0] += jnp.where(mc, low, zero)
            A[L, 2, 2] += jnp.where(mc, zero, low)
            A[L, 0, 1] += jnp.where(mr, term[1], zero)
            A[L, 2, 1] += jnp.where(mr, zero, term[1])
        else:
            A[L, 1, 0] += jnp.where(mc, term[0], zero)
            A[L, 1, 2] += jnp.where(mc, zero, term[0])
            A[L, 1, 1] += term[1]

    local[0].wait()

    def roll_probe(p, carry):
        power = None
        for plane in range(2):
            x = pltpu.roll(probe[plane], off_ref[0, p], 0)
            x = pltpu.roll(x, off_ref[1, p], 1)
            rolled[p, plane] = x
            power = x * x if power is None else power + x * x
        for i in range(2):
            rows = power[i * T:(i + 1) * T]
            add_rows(2 * ITERS, p, i, [rows[:, :T], rows[:, T:]])
        return carry

    lax.fori_loop(0, n_pos, roll_probe, 0)
    light = ITERS
    f_begin(light)

    local[1].wait()
    lane_in = lax.broadcasted_iota(jnp.int32, (W, W), 0)
    lane_out = lax.broadcasted_iota(jnp.int32, (W, W), 1)
    source = jnp.where(lane_out < T, 2 * lane_out, 2 * lane_out - (W - 1))
    perm = jnp.where(lane_in == source, 1.0, 0.0).astype(bf16)

    def permute_amp(p, carry):
        x = amp[p]
        hi = x.astype(bf16)
        mid, low = split(x - hi.astype(f32))
        x = mm(hi, perm) + mm(mid, perm) + mm(low, perm)
        for half in range(2):
            lanes = pl.ds(half * T, T)
            halves[half] = x[:, half * T:(half + 1) * T]
            for par in range(2):
                ampp[p, par, :, lanes] = halves[half, pl.ds(par, T, stride=2), :]
        return carry

    lax.fori_loop(0, n_pos, permute_amp, 0)
    local[2].wait()

    def right(x, m):
        hi, lo = split(x)
        return mm(hi, mats[m]) + mm(lo, mats[m]) + mm(hi, mats[m + 1])

    def left(m, x):
        hi, lo = split(x)
        return mm(mats[m], hi) + mm(mats[m + 1], hi) + mm(mats[m], lo)

    def exit_rows(it, p, i):
        mr = row_of >= off_ref[0, p]
        mc = col_of >= off_ref[1, p]
        ob = []
        for L in (2 * it, 2 * it + 1):
            t = lambda a, b: G[L, a, b]
            if i == 0:
                ob.append([
                    jnp.where(mr, jnp.where(mc, t(0, 0), t(0, 2)), jnp.where(mc, t(2, 0), t(2, 2))),
                    jnp.where(mr, t(0, 1), t(2, 1)),
                ])
            else:
                ob.append([jnp.where(mc, t(1, 0), t(1, 2)), t(1, 1)])
        rows = slice(i * T, (i + 1) * T)
        pr = [rolled[p, 0, rows, :T], rolled[p, 0, rows, T:]]
        pi = [rolled[p, 1, rows, :T], rolled[p, 1, rows, T:]]
        er = [pr[j] * ob[0][j] - pi[j] * ob[1][j] for j in range(2)]
        ei = [pr[j] * ob[1][j] + pi[j] * ob[0][j] for j in range(2)]
        u = jnp.concatenate([er[0] + er[1], ei[0] + ei[1]], 1)
        v = jnp.concatenate([er[0] - er[1], ei[0] - ei[1]], 1)
        return right(u, 0), right(v, 2)

    def back_rows(zr, zi):
        even = right(jnp.concatenate([zr[:, :T], zi[:, :T]], 1), 4)
        odd = right(jnp.concatenate([zr[:, T:], zi[:, T:]], 1), 6)
        return even, odd

    def terms(p, i, even, odd):
        tot, dif = even + odd, even - odd
        br = [tot[:, :T], dif[:, :T]]
        bi = [tot[:, T:], dif[:, T:]]
        rows = slice(i * T, (i + 1) * T)
        pr = [rolled[p, 0, rows, :T], rolled[p, 0, rows, T:]]
        pi = [rolled[p, 1, rows, :T], rolled[p, 1, rows, T:]]
        return (
            [pr[j] * br[j] + pi[j] * bi[j] for j in range(2)],
            [pr[j] * bi[j] - pi[j] * br[j] for j in range(2)],
        )

    def before(it, p):
        even, odd = exit_rows(it, p, 1)
        yield
        held[p, 0] = even
        held[p, 1] = odd
        yield

    def window(it, p):
        even, odd = exit_rows(it, p, 0)
        yield
        low_even, low_odd = held[p, 0], held[p, 1]
        yr = [jnp.concatenate([e[:, :T], o[:, :T]], 1) for e, o in ((even, odd), (low_even, low_odd))]
        yi = [jnp.concatenate([e[:, T:], o[:, T:]], 1) for e, o in ((even, odd), (low_even, low_odd))]
        u = jnp.concatenate([yr[0] + yr[1], yi[0] + yi[1]], 0)
        v = jnp.concatenate([yr[0] - yr[1], yi[0] - yi[1]], 0)
        back = []
        fars = [left(4 + 2 * par, x) for par, x in ((0, u), (1, v))]
        yield
        for par, far in enumerate(fars):
            fr, fi = far[:T], far[T:]
            keep = 1.0 - ampp[p, par] * lax.rsqrt(jnp.maximum(fr * fr + fi * fi, 0.25))
            back.append(left(2 * par, jnp.concatenate([fr * keep, fi * keep], 0)))
        yield
        tot, dif = back[0] + back[1], back[0] - back[1]
        held[p, 0] = dif[:T]
        held[p, 1] = dif[T:]
        even, odd = back_rows(tot[:T], tot[T:])
        yield
        for L, term in zip((2 * it, 2 * it + 1), terms(p, 0, even, odd)):
            add_rows(L, p, 0, term)
        yield

    def after(it, p):
        even, odd = back_rows(held[p, 0], held[p, 1])
        yield
        for L, term in zip((2 * it, 2 * it + 1), terms(p, 1, even, odd)):
            add_rows(L, p, 1, term)
        yield

    def every(part, stages, it):
        def step(t, carry):
            running = [part(it, GROUP * t + i) for i in range(GROUP)]
            for _ in range(stages):
                for one in running:
                    next(one)
            return carry

        lax.fori_loop(0, n_pos // GROUP, step, 0)

    g_finish(0, lambda: f_core(light))
    f_across(light)
    for it in range(ITERS):
        every(window, 5, it)
        f_begin(it)
        every(after, 2, it)
        if it == 0:
            for L, q in chunks(light):
                ill[pl.ds(q * CHUNK, CHUNK)] = f_end(light, L, q) + 1.0
        f_core(it)
        if it == ITERS - 1:
            drain(f_copy, f_sends, light)
            for done in range(ITERS):
                drain(g_copy, g_sends, done)
            for done in range(ITERS - 1):
                drain(f_copy, f_sends, done)
        f_across(it)
        for L, q in chunks(it):
            part = pl.ds(q * CHUNK, CHUNK)
            new = G[L, 1, 1, part] - f_end(it, L, q) / ill[part]
            if it < ITERS - 1:
                G[L + 2, 1, 1, part] = new
                g_copy(it + 1, 1, L + 2, q).start()
            else:
                out_ref[L - 2 * it, part] = new
        if it < ITERS - 1:
            g_begin(it + 1)
            g_finish(it + 1)
    drain(f_copy, f_sends, ITERS - 1)


def local(n_rows, n_cols, object_field, probe, amplitudes, offsets):
    n_pos = amplitudes.shape[2]
    n = 2 * ITERS

    def fix(x):
        return pltpu.with_memory_space_constraint(x, pltpu.HBM)

    hbm = pl.BlockSpec(memory_space=pltpu.HBM)
    vmem = pl.BlockSpec(memory_space=pltpu.VMEM)
    return pl.pallas_call(
        functools.partial(kernel, n_rows, n_cols, n_pos),
        out_shape=jax.ShapeDtypeStruct(object_field.shape, f32),
        in_specs=[hbm, pl.BlockSpec(memory_space=pltpu.SMEM), hbm, hbm, hbm],
        out_specs=vmem,
        scratch_shapes=[
            pltpu.VMEM((n, 3, 3, T, T), f32),
            pltpu.VMEM((n + 1, 3, 3, T, T), f32),
            pltpu.VMEM((n + 1, 3, T, T), f32),
            pltpu.VMEM((n + 1, 3, T, T), f32),
            pltpu.VMEM((n + 1, T, T), f32),
            pltpu.VMEM((n + 1, T, T), f32),
            pltpu.VMEM((T, T), f32),
            pltpu.VMEM((2, W, W), f32),
            pltpu.VMEM((n_pos, W, W), f32),
            pltpu.VMEM((8, W, W), bf16),
            pltpu.VMEM((n_pos, 2, W, W), f32),
            pltpu.VMEM((n_pos, 2, T, W), f32),
            pltpu.VMEM((2, W, T), f32),
            pltpu.VMEM((n_pos, 2, T, W), f32),
            pltpu.SemaphoreType.DMA((ITERS, 8)),
            pltpu.SemaphoreType.DMA((n, 8, T // CHUNK)),
            pltpu.SemaphoreType.DMA((ITERS + 1, 8)),
            pltpu.SemaphoreType.DMA((n + 1, 8, T // CHUNK)),
            pltpu.SemaphoreType.DMA((5,)),
        ],
        compiler_params=pltpu.CompilerParams(
            collective_id=0, has_side_effects=True, vmem_limit_bytes=VMEM_MIB * 1024 * 1024
        ),
    )(
        fix(object_field),
        fix(offsets[0, 0].T),
        fix(probe),
        fix(amplitudes[0, 0]),
        fix(jnp.asarray(dft_parts())),
    )


def solution(mesh):
    placed = (
        P(None, "rows", "cols"),
        P(),
        P("rows", "cols", None, None, None),
        P("rows", "cols", None, None),
    )
    body = functools.partial(local, mesh.shape["rows"], mesh.shape["cols"])
    return jax.shard_map(
        body, mesh=mesh, in_specs=placed, out_specs=P(None, "rows", "cols"), check_vma=False
    )
```

```python
import functools
import math

import jax
import jax.numpy as jnp
import numpy as np
from jax import lax
from jax.experimental import pallas as pl
from jax.experimental.pallas import tpu as pltpu
from jax.sharding import PartitionSpec as P

ITERS = 2
T = 128
W = 256
CHUNK = 64
GROUP = 4
VMEM_MIB = 28
MESH = pl.DeviceIdType.MESH
f32 = jnp.float32
bf16 = jnp.bfloat16


def dft_parts():
    m = np.arange(T)
    mats = []
    for odd in (0, 1):
        turns = (m[:, None] * (2 * m[None, :] + odd)) % W
        angle = 2.0 * np.pi / W * turns
        c, s = np.cos(angle) / 16.0, np.sin(angle) / 16.0
        mats.append(np.block([[c, -s], [s, c]]))
    mats = [mats[0], mats[1], mats[0].T, mats[1].T]
    out = []
    for a in mats:
        a = a.astype(np.float32)
        hi = a.astype(jnp.bfloat16)
        lo = (a - hi.astype(np.float32)).astype(jnp.bfloat16)
        out += [hi, lo]
    return np.stack(out)


def split(x):
    hi = x.astype(bf16)
    return hi, (x - hi.astype(f32)).astype(bf16)


def mm(a, b):
    return jnp.dot(a, b, preferred_element_type=f32)


def kernel(
    n_rows, n_cols, n_pos,
    obj_hbm, off_ref, probe_hbm, amp_hbm, mats_hbm,
    out_ref,
    G, A, FC, FR, FX, FY, ill, probe, amp, mats, rolled, ampp, halves, held,
    g_send, g_recv, f_send, f_recv, l_sem,
):
    r = lax.axis_index("rows")
    c = lax.axis_index("cols")
    ro, h = lax.rem(r, 2), lax.rem(c, 2)
    rc, rx = r + 1 - 2 * ro, r - 1 + 2 * ro
    cp = c + 1 - 2 * h
    cx, cf = c + 2 - 4 * h, c - 2 + 4 * h
    has_x = (rx >= 0) & (rx < n_rows)
    has_cx = (cx >= 0) & (cx < n_cols)
    has_far = (cf >= 0) & (cf < n_cols)
    rcs = rc - r + 1
    rxs = 2 - rcs
    hp = cp - c + 1
    fp = 2 - hp

    barrier = pltpu.get_barrier_semaphore()

    def greet(row, col):
        pl.semaphore_signal(
            barrier, inc=1, device_id={"rows": row, "cols": col}, device_id_type=MESH
        )

    @pl.when(has_cx)
    def _():
        greet(r, cx)

    @pl.when(has_far)
    def _():
        greet(r, cf)

    greet(r, cp)

    @pl.when(has_x)
    def _():
        greet(rx, c)
        greet(rx, cp)

    greet(rc, c)

    local = [
        pltpu.make_async_copy(probe_hbm, probe, l_sem.at[0]),
        pltpu.make_async_copy(amp_hbm, amp, l_sem.at[1]),
        pltpu.make_async_copy(mats_hbm, mats, l_sem.at[2]),
        pltpu.make_async_copy(obj_hbm.at[0], G.at[0, 1, 1], l_sem.at[3]),
        pltpu.make_async_copy(obj_hbm.at[1], G.at[1, 1, 1], l_sem.at[4]),
    ]
    for i in (3, 4, 0, 1, 2):
        local[i].start()

    always = None

    def both(a, b):
        return a & b

    def when(cond, f):
        if cond is None:
            f()
        else:
            pl.when(cond)(f)

    def tile(ph, L, q):
        if L is None:
            n = 2 if ph < ITERS else 1
            return pl.ds(2 * ph, n), ()
        return L, (pl.ds(q * CHUNK, CHUNK),)

    def chunks(ph):
        n = 2 if ph < ITERS else 1
        return [(2 * ph + i, q) for i in range(n) for q in range(T // CHUNK)]

    def remote(src, dst, send, recv, ph, L, q, k, dev):
        return pltpu.make_async_remote_copy(
            src_ref=src,
            dst_ref=dst,
            send_sem=send.at[ph, k],
            recv_sem=recv.at[2 * ph, k, 0] if L is None else recv.at[L, k, q],
            device_id={"rows": dev[0], "cols": dev[1]},
            device_id_type=MESH,
        )

    g_sends = {2: has_x, 3: has_x, 4: has_cx, 5: both(has_x, has_far), 7: has_far}

    def g_copy(ph, k, L=None, q=None):
        src, dst, dev = {
            0: ((1, 1), (2 - rcs, 1), (rc, c)),
            1: ((1, 1), (1, 2 - hp), (r, cp)),
            2: ((1, 1), (2 - rxs, 1), (rx, c)),
            3: ((1, 1), (2 - rxs, 2 - hp), (rx, cp)),
            4: ((1, hp), (1, fp), (r, cx)),
            5: ((1, fp), (2 - rxs, fp), (rx, c)),
            6: ((1, hp), (2 - rcs, hp), (rc, c)),
            7: ((1, fp), (2 - rcs, fp), (rc, c)),
        }[k]
        lead, part = tile(ph, L, q)
        return remote(
            G.at[(lead,) + src + part], G.at[(lead,) + dst + part], g_send, g_recv, ph, L, q, k, dev
        )

    def g_begin(ph):
        g_copy(ph, 0).start()

        @pl.when(has_x)
        def _():
            g_copy(ph, 3).start()


    def g_finish(ph, meanwhile=None):
        for L, q in chunks(ph):
            g_copy(ph, 1, L, q).wait_recv()
            pl.when(has_cx)(lambda: g_copy(ph, 4, L, q).start())
        g_copy(ph, 6).start()
        pl.when(has_x)(lambda: g_copy(ph, 2).start())
        if meanwhile is not None:
            meanwhile()

        @pl.when(has_far)
        def _():
            for L, q in chunks(ph):
                g_copy(ph, 4, L, q).wait_recv()
                pl.when(has_x)(lambda: g_copy(ph, 5, L, q).start())
                g_copy(ph, 7, L, q).start()

        every(before, 2, ph)
        g_copy(ph, 0).wait_recv()
        g_copy(ph, 6).wait_recv()

        @pl.when(has_x)
        def _():
            g_copy(ph, 2).wait_recv()
            g_copy(ph, 3).wait_recv()

        @pl.when(has_far)
        def _():
            for L, q in chunks(ph):
                g_copy(ph, 7, L, q).wait_recv()
                pl.when(has_x)(lambda: g_copy(ph, 5, L, q).wait_recv())

    f_sends = {1: has_far, 2: has_x, 4: has_x, 5: has_x}

    def f_copy(ph, k, L=None, q=None):
        lead, part = tile(ph, L, q)
        src, dst, dev = {
            0: (A.at[(lead, rcs, fp) + part], FC.at[(lead, fp) + part], (rc, c)),
            6: (A.at[(lead, rcs, hp) + part], FC.at[(lead, hp) + part], (rc, c)),
            7: (A.at[(lead, rcs, 1) + part], FC.at[(lead, 1) + part], (rc, c)),
            2: (A.at[(lead, rxs, fp) + part], FR.at[(lead, fp) + part], (rx, c)),
            5: (A.at[(lead, rxs, hp) + part], FR.at[(lead, 2 - hp) + part], (rx, cp)),
            4: (A.at[(lead, rxs, 1) + part], FR.at[(lead, 1) + part], (rx, c)),
            1: (A.at[(lead, 1, fp) + part], FX.at[(lead,) + part], (r, cf)),
            3: (A.at[(lead, 1, hp) + part], FY.at[(lead,) + part], (r, cp)),
        }[k]
        return remote(src, dst, f_send, f_recv, ph, L, q, k, dev)

    def f_begin(ph):
        @pl.when(has_x)
        def _():
            for L, q in chunks(ph):
                f_copy(ph, 2, L, q).start()
            f_copy(ph, 5).start()

        for L, q in chunks(ph):
            f_copy(ph, 0, L, q).start()
        f_copy(ph, 6).start()
        f_copy(ph, 7).start()

    def f_core(ph):
        for L, q in chunks(ph):
            part = pl.ds(q * CHUNK, CHUNK)
            f_copy(ph, 0, L, q).wait_recv()
            pl.when(has_x)(lambda: f_copy(ph, 2, L, q).wait_recv())
            A[L, 1, fp, part] += FC[L, fp, part] + FR[L, fp, part]
            pl.when(has_far)(lambda: f_copy(ph, 1, L, q).start())
        pl.when(has_x)(lambda: f_copy(ph, 4).start())
        f_copy(ph, 6).wait_recv()
        for L, q in chunks(ph):
            part = pl.ds(q * CHUNK, CHUNK)
            A[L, 1, hp, part] += FC[L, hp, part]

    def f_across(ph):
        for L, q in chunks(ph):
            part = pl.ds(q * CHUNK, CHUNK)
            pl.when(has_cx)(lambda: f_copy(ph, 1, L, q).wait_recv())
            A[L, 1, hp, part] += FX[L, part]
            f_copy(ph, 3, L, q).start()
        f_copy(ph, 7).wait_recv()

        @pl.when(has_x)
        def _():
            f_copy(ph, 4).wait_recv()
            f_copy(ph, 5).wait_recv()

        for L, q in chunks(ph):
            part = pl.ds(q * CHUNK, CHUNK)
            A[L, 1, 1, part] += FC[L, 1, part] + FR[L, 1, part] + FR[L, hp, part]

    def f_end(ph, L, q):
        part = pl.ds(q * CHUNK, CHUNK)
        f_copy(ph, 3, L, q).wait_recv()
        return A[L, 1, 1, part] + FY[L, part]

    def drain(copy, sends, ph):
        for k in range(8):
            when(sends.get(k, always), lambda: copy(ph, k).wait_send())

    local[3].wait()
    local[4].wait()
    greeted = 2 + 2 * has_x.astype(jnp.int32) + has_cx.astype(jnp.int32) + has_far.astype(jnp.int32)
    pl.semaphore_wait(barrier, greeted)
    for L, q in chunks(0):
        g_copy(0, 1, L, q).start()
    g_begin(0)

    zero_tile = jnp.zeros((T, T), f32)

    @pl.when(jnp.logical_not(has_x))
    def _():
        for L in range(2 * ITERS):
            for col in range(3):
                G[L, rxs, col] = zero_tile
        for L in range(2 * ITERS + 1):
            for col in range(3):
                FR[L, col] = zero_tile

    @pl.when(jnp.logical_not(has_cx))
    def _():
        for L in range(2 * ITERS + 1):
            FX[L] = zero_tile

    @pl.when(jnp.logical_not(has_far))
    def _():
        for L in range(2 * ITERS):
            for row in range(3):
                G[L, row, fp] = zero_tile

    for L in range(2 * ITERS + 1):
        for row in range(3):
            for col in range(3):
                A[L, row, col] = zero_tile

    row_of = lax.broadcasted_iota(jnp.int32, (T, T), 0)
    col_of = lax.broadcasted_iota(jnp.int32, (T, T), 1)

    def add_rows(L, p, i, term):
        mr = row_of >= off_ref[0, p]
        mc = col_of >= off_ref[1, p]
        zero = jnp.zeros((T, T), f32)
        if i == 0:
            top = jnp.where(mr, term[0], zero)
            low = jnp.where(mr, zero, term[0])
            A[L, 0, 0] += jnp.where(mc, top, zero)
            A[L, 0, 2] += jnp.where(mc, zero, top)
            A[L, 2, 0] += jnp.where(mc, low, zero)
            A[L, 2, 2] += jnp.where(mc, zero, low)
            A[L, 0, 1] += jnp.where(mr, term[1], zero)
            A[L, 2, 1] += jnp.where(mr, zero, term[1])
        else:
            A[L, 1, 0] += jnp.where(mc, term[0], zero)
            A[L, 1, 2] += jnp.where(mc, zero, term[0])
            A[L, 1, 1] += term[1]

    local[0].wait()

    def roll_probe(p, carry):
        power = None
        for plane in range(2):
            x = pltpu.roll(probe[plane], off_ref[0, p], 0)
            x = pltpu.roll(x, off_ref[1, p], 1)
            rolled[p, plane] = x
            power = x * x if power is None else power + x * x
        for i in range(2):
            rows = power[i * T:(i + 1) * T]
            add_rows(2 * ITERS, p, i, [rows[:, :T], rows[:, T:]])
        return carry

    lax.fori_loop(0, n_pos, roll_probe, 0)
    light = ITERS
    f_begin(light)

    local[1].wait()
    lane_in = lax.broadcasted_iota(jnp.int32, (W, W), 0)
    lane_out = lax.broadcasted_iota(jnp.int32, (W, W), 1)
    source = jnp.where(lane_out < T, 2 * lane_out, 2 * lane_out - (W - 1))
    perm = jnp.where(lane_in == source, 1.0, 0.0).astype(bf16)

    def permute_amp(p, carry):
        x = amp[p]
        hi = x.astype(bf16)
        mid, low = split(x - hi.astype(f32))
        x = mm(hi, perm) + mm(mid, perm) + mm(low, perm)
        for half in range(2):
            lanes = pl.ds(half * T, T)
            halves[half] = x[:, half * T:(half + 1) * T]
            for par in range(2):
                ampp[p, par, :, lanes] = halves[half, pl.ds(par, T, stride=2), :]
        return carry

    lax.fori_loop(0, n_pos, permute_amp, 0)
    local[2].wait()

    def right(x, m):
        hi, lo = split(x)
        return mm(hi, mats[m]) + mm(lo, mats[m]) + mm(hi, mats[m + 1])

    def left(m, x):
        hi, lo = split(x)
        return mm(mats[m], hi) + mm(mats[m + 1], hi) + mm(mats[m], lo)

    def exit_rows(it, p, i):
        mr = row_of >= off_ref[0, p]
        mc = col_of >= off_ref[1, p]
        ob = []
        for L in (2 * it, 2 * it + 1):
            t = lambda a, b: G[L, a, b]
            if i == 0:
                ob.append([
                    jnp.where(mr, jnp.where(mc, t(0, 0), t(0, 2)), jnp.where(mc, t(2, 0), t(2, 2))),
                    jnp.where(mr, t(0, 1), t(2, 1)),
                ])
            else:
                ob.append([jnp.where(mc, t(1, 0), t(1, 2)), t(1, 1)])
        rows = slice(i * T, (i + 1) * T)
        pr = [rolled[p, 0, rows, :T], rolled[p, 0, rows, T:]]
        pi = [rolled[p, 1, rows, :T], rolled[p, 1, rows, T:]]
        er = [pr[j] * ob[0][j] - pi[j] * ob[1][j] for j in range(2)]
        ei = [pr[j] * ob[1][j] + pi[j] * ob[0][j] for j in range(2)]
        u = jnp.concatenate([er[0] + er[1], ei[0] + ei[1]], 1)
        v = jnp.concatenate([er[0] - er[1], ei[0] - ei[1]], 1)
        return right(u, 0), right(v, 2)

    def back_rows(zr, zi):
        even = right(jnp.concatenate([zr[:, :T], zi[:, :T]], 1), 4)
        odd = right(jnp.concatenate([zr[:, T:], zi[:, T:]], 1), 6)
        return even, odd

    def terms(p, i, even, odd):
        tot, dif = even + odd, even - odd
        br = [tot[:, :T], dif[:, :T]]
        bi = [tot[:, T:], dif[:, T:]]
        rows = slice(i * T, (i + 1) * T)
        pr = [rolled[p, 0, rows, :T], rolled[p, 0, rows, T:]]
        pi = [rolled[p, 1, rows, :T], rolled[p, 1, rows, T:]]
        return (
            [pr[j] * br[j] + pi[j] * bi[j] for j in range(2)],
            [pr[j] * bi[j] - pi[j] * br[j] for j in range(2)],
        )

    def before(it, p):
        even, odd = exit_rows(it, p, 1)
        yield
        held[p, 0] = even
        held[p, 1] = odd
        yield

    def window(it, p):
        even, odd = exit_rows(it, p, 0)
        yield
        low_even, low_odd = held[p, 0], held[p, 1]
        yr = [jnp.concatenate([e[:, :T], o[:, :T]], 1) for e, o in ((even, odd), (low_even, low_odd))]
        yi = [jnp.concatenate([e[:, T:], o[:, T:]], 1) for e, o in ((even, odd), (low_even, low_odd))]
        u = jnp.concatenate([yr[0] + yr[1], yi[0] + yi[1]], 0)
        v = jnp.concatenate([yr[0] - yr[1], yi[0] - yi[1]], 0)
        back = []
        fars = [left(4 + 2 * par, x) for par, x in ((0, u), (1, v))]
        yield
        for par, far in enumerate(fars):
            fr, fi = far[:T], far[T:]
            keep = 1.0 - ampp[p, par] * lax.rsqrt(jnp.maximum(fr * fr + fi * fi, 0.25))
            back.append(left(2 * par, jnp.concatenate([fr * keep, fi * keep], 0)))
        yield
        tot, dif = back[0] + back[1], back[0] - back[1]
        held[p, 0] = dif[:T]
        held[p, 1] = dif[T:]
        even, odd = back_rows(tot[:T], tot[T:])
        yield
        for L, term in zip((2 * it, 2 * it + 1), terms(p, 0, even, odd)):
            add_rows(L, p, 0, term)
        yield

    def after(it, p):
        even, odd = back_rows(held[p, 0], held[p, 1])
        yield
        for L, term in zip((2 * it, 2 * it + 1), terms(p, 1, even, odd)):
            add_rows(L, p, 1, term)
        yield

    def every(part, stages, it):
        def step(t, carry):
            running = [part(it, GROUP * t + i) for i in range(GROUP)]
            for _ in range(stages):
                for one in running:
                    next(one)
            return carry

        lax.fori_loop(0, n_pos // GROUP, step, 0)

    g_finish(0, lambda: f_core(light))
    f_across(light)
    for it in range(ITERS):
        every(window, 5, it)
        f_begin(it)
        every(after, 2, it)
        if it == 0:
            for L, q in chunks(light):
                ill[pl.ds(q * CHUNK, CHUNK)] = f_end(light, L, q) + 1.0
        f_core(it)
        if it == ITERS - 1:
            drain(f_copy, f_sends, light)
            for done in range(ITERS):
                drain(g_copy, g_sends, done)
            for done in range(ITERS - 1):
                drain(f_copy, f_sends, done)
        f_across(it)
        for L, q in chunks(it):
            part = pl.ds(q * CHUNK, CHUNK)
            new = G[L, 1, 1, part] - f_end(it, L, q) / ill[part]
            if it < ITERS - 1:
                G[L + 2, 1, 1, part] = new
                g_copy(it + 1, 1, L + 2, q).start()
            else:
                out_ref[L - 2 * it, part] = new
        if it < ITERS - 1:
            g_begin(it + 1)
            g_finish(it + 1)
    drain(f_copy, f_sends, ITERS - 1)


def local(n_rows, n_cols, object_field, probe, amplitudes, offsets):
    n_pos = amplitudes.shape[2]
    n = 2 * ITERS

    def fix(x):
        return pltpu.with_memory_space_constraint(x, pltpu.HBM)

    hbm = pl.BlockSpec(memory_space=pltpu.HBM)
    vmem = pl.BlockSpec(memory_space=pltpu.VMEM)
    return pl.pallas_call(
        functools.partial(kernel, n_rows, n_cols, n_pos),
        out_shape=jax.ShapeDtypeStruct(object_field.shape, f32),
        in_specs=[hbm, pl.BlockSpec(memory_space=pltpu.SMEM), hbm, hbm, hbm],
        out_specs=vmem,
        scratch_shapes=[
            pltpu.VMEM((n, 3, 3, T, T), f32),
            pltpu.VMEM((n + 1, 3, 3, T, T), f32),
            pltpu.VMEM((n + 1, 3, T, T), f32),
            pltpu.VMEM((n + 1, 3, T, T), f32),
            pltpu.VMEM((n + 1, T, T), f32),
            pltpu.VMEM((n + 1, T, T), f32),
            pltpu.VMEM((T, T), f32),
            pltpu.VMEM((2, W, W), f32),
            pltpu.VMEM((n_pos, W, W), f32),
            pltpu.VMEM((8, W, W), bf16),
            pltpu.VMEM((n_pos, 2, W, W), f32),
            pltpu.VMEM((n_pos, 2, T, W), f32),
            pltpu.VMEM((2, W, T), f32),
            pltpu.VMEM((n_pos, 2, T, W), f32),
            pltpu.SemaphoreType.DMA((ITERS, 8)),
            pltpu.SemaphoreType.DMA((n, 8, T // CHUNK)),
            pltpu.SemaphoreType.DMA((ITERS + 1, 8)),
            pltpu.SemaphoreType.DMA((n + 1, 8, T // CHUNK)),
            pltpu.SemaphoreType.DMA((5,)),
        ],
        compiler_params=pltpu.CompilerParams(
            collective_id=0, has_side_effects=True, vmem_limit_bytes=VMEM_MIB * 1024 * 1024
        ),
    )(
        fix(object_field),
        fix(offsets[0, 0].T),
        fix(probe),
        fix(amplitudes[0, 0]),
        fix(jnp.asarray(dft_parts())),
    )


def solution(mesh):
    placed = (
        P(None, "rows", "cols"),
        P(),
        P("rows", "cols", None, None, None),
        P("rows", "cols", None, None),
    )
    body = functools.partial(local, mesh.shape["rows"], mesh.shape["cols"])
    return jax.shard_map(
        body, mesh=mesh, in_specs=placed, out_specs=P(None, "rows", "cols"), check_vma=False
    )
```
